32 devices in a mesh: expert: 16 (over z, x, core), dp: 2 (over y).
Axes of the slice: x: 2, y: 2, z: 4, core: 2. Of those that a mesh axis runs over, the one named last changes fastest.
Arguments:
- tokens: bfloat16 [4096, 2560], P(('expert', 'dp')), may hold values from -6 to 6
- routes: int32 [4096, 2], P(('expert', 'dp')), may hold values from 0 to 3, all different within a row; in each aligned block of 128 rows (0 to 127, 128 to 255, ...) at most 88 rows name the same one
- combine_weight: float32 [4096, 2], P(('expert', 'dp')), may hold values from 0.05 to 1
- owner_plan: int32 [4], replicated, may hold values from 0 to 3, as said below
- w_in: bfloat16 [2, 3072, 2560], P(None, 'expert', 'dp'), may hold values from -0.125 to 0.125
- w_out: bfloat16 [3072, 2560], P('expert', 'dp'), may hold values from -0.21875 to 0.21875
- grad_in: bfloat16 [2, 2, 3072, 2560], P('dp', None, 'expert'), may hold values from -6 to 6
- grad_out: bfloat16 [2, 3072, 2560], P('dp', 'expert'), may hold values from -6 to 6
- first_in: bfloat16 [2, 3072, 2560], P(None, 'expert', 'dp'), may hold values from -3 to 3
- second_in: bfloat16 [2, 3072, 2560], P(None, 'expert', 'dp'), may hold values from 0.25 to 4
- first_out: bfloat16 [3072, 2560], P('expert', 'dp'), may hold values from -3 to 3
- second_out: bfloat16 [3072, 2560], P('expert', 'dp'), may hold values from 0.25 to 4
Outputs:
- combined: bfloat16 [4096, 2560], P(('expert', 'dp'))
- first_in_next: bfloat16 [2, 3072, 2560], P(None, 'expert', 'dp')
- second_in_next: bfloat16 [2, 3072, 2560], P(None, 'expert', 'dp')
- first_out_next: bfloat16 [3072, 2560], P('expert', 'dp')
- second_out_next: bfloat16 [3072, 2560], P('expert', 'dp')
The draws below stay inside these ranges and needn't reach their ends.
Inputs may be any that keep to these rules, and one draw needn't show every extreme that they name: owner_plan is an involution: exactly 2 pairs of experts trade owners, every other expert maps to itself. `routes`: in the rows of one device (128 rows) no expert is named by more than 88 rows, a bound that some expert reaches in some device.
All inputs are finite; a program needn't handle non-finite values.
Results may differ from the reference program's by a relative error of at most 0.014.
Values may be sent and summed in bfloat16 or wider, within the bound.
A program may use at most 192 MiB of HBM per device.

```python
import math
import jax
import jax.numpy as jnp
import numpy as np
from jax import lax

D = 2560
HID = 768
GROUP = 4
TOK_DEV = 128
HDEV = 192
EXPERTS = 4
TOP = 2
MOVED = 2
CAP = 88
TOKENS = 4096
N_DP = 2
DEVICES = 32


def draw_owner_plan(key, part):
    shuffled = jax.random.permutation(jax.random.fold_in(key, 7), EXPERTS).astype(jnp.int32)
    expert_ids = jnp.arange(EXPERTS, dtype=jnp.int32)
    leaving = shuffled[:MOVED]
    arriving = shuffled[MOVED:2 * MOVED]
    owner_plan = expert_ids.at[leaving].set(arriving).at[arriving].set(leaving)
    return owner_plan.astype(jnp.int32)


def shard_levels(stream_key, dims, cuts, low, top_value):
    factor_of = 1.0
    for axis_at, parts in cuts:
        heights = jax.random.uniform(jax.random.fold_in(jax.random.fold_in(stream_key, 6), axis_at), (parts,), jnp.float32, low / len(cuts), top_value / len(cuts))
        factor_of = factor_of * jnp.repeat(jnp.exp(heights), dims[axis_at] // parts).reshape((-1,) + (1,) * (len(dims) - 1 - axis_at))
    return factor_of


def deal_out(key, own, number, rows, number_of, top, bound, slope):
    order = jax.random.permutation(key, number_of)
    packed, common = portions_of(number_of, rows * top, bound, slope, True), portions_of(number_of, rows * top, bound, slope, False)
    places = jnp.arange(number_of)

    def named(lengths, offset_by):
        used = int((lengths > 0).sum())
        fixed = max(1, used // 4)
        moved = fixed + (places - fixed + offset_by * (used - fixed)) % max(1, number_of - fixed)
        return jnp.zeros((number_of,), jnp.int32).at[order[jnp.where(places < fixed, places, moved)]].set(jnp.asarray(lengths, jnp.int32))

    lengths = jnp.where(number % 4 == 0, named(packed, number // 4), named(common, number - number // 4 - 1))
    mixed = jax.random.permutation(jax.random.fold_in(own, 3), number_of)
    giver, taker = mixed[0:number_of // 2 * 2:2], mixed[1:number_of // 2 * 2:2]
    slack = jnp.minimum(lengths[giver] - 1, bound - lengths[taker]) // 2
    slack = jnp.where((giver == order[0]) | (taker == order[0]) | (lengths[taker] == 0), 0, jnp.maximum(slack, 0))
    moved = jax.random.randint(jax.random.fold_in(own, 4), (number_of // 2,), 0, 1 << 20) % (slack + 1)
    lengths = lengths.at[giver].add(-moved).at[taker].add(moved)
    members = jnp.searchsorted(jnp.cumsum(lengths), jnp.arange(rows * top), side="right").astype(jnp.int32)
    listing = members.reshape(top, rows).T
    listing = listing[jax.random.permutation(jax.random.fold_in(own, 1), rows)]
    offset_by = jax.random.randint(jax.random.fold_in(own, 2), (rows, 1), 0, top)
    return jnp.take_along_axis(listing, (jnp.arange(top)[None, :] + offset_by) % top, axis=1)


def portions_of(amount, total, bound, slope, full):
    loads = [(1 << 20) // math.isqrt(rank ** slope) + 1 for rank in range(1, amount + 1)]
    largest = bound if full else min(bound, max(-(-total // amount), total * loads[0] // sum(loads)))
    least = 1 if total - largest >= amount - 1 else 0
    counts, rest = [largest] + [least] * (amount - 1), total - largest - least * (amount - 1)
    while rest > 0:
        candidates = [i for i in range(1, amount) if counts[i] < largest] or [i for i in range(1, amount) if counts[i] < bound]
        pool, left = sum([loads[i] for i in candidates]), rest
        for i in candidates:
            extra = min(bound - counts[i], max(1, left * loads[i] // pool), rest)
            counts[i] = counts[i] + extra
            rest = rest - extra
    return np.array(counts)


def noise(rng, extent, scale, limit, shards=(), held_as=jnp.bfloat16):
    array = jax.random.normal(rng, extent, jnp.float32) * scale
    if len(shards) > 0:
        array = shard_levels(rng, extent, shards, -0.22, 0.18) * array
    return jnp.clip(array, min=-limit, max=limit).astype(held_as)


def setup_inputs(seed: int = 0) -> dict:
    keys = jax.random.split(jax.random.key(seed), 13)
    tokens = noise(keys[0], (TOKENS, D), 1.0, 6.0, ((0, 32),))
    routes_keys = jax.random.split(jax.random.fold_in(keys[1], 1), TOKENS // TOK_DEV)
    routes_turns = jax.random.permutation(jax.random.fold_in(keys[1], 3), TOKENS // TOK_DEV)
    routes = jax.vmap(lambda own, number: deal_out(jax.random.fold_in(keys[1], 2), own, number, TOK_DEV, EXPERTS, TOP, CAP, 2))(routes_keys, routes_turns).reshape((TOKENS, TOP))
    combine_weight = jnp.clip(jnp.exp(math.log(1.0) - 2.9957323 * jax.random.uniform(keys[2], (TOKENS, TOP), jnp.float32) ** shard_levels(keys[2], (TOKENS, TOP), ((0, 32),), -0.2, 0.2)), 0.05, 1.0)
    owner_plan = draw_owner_plan(jax.random.fold_in(keys[12], 71), 0)
    w_in = noise(keys[4], (2, EXPERTS * HID, D), D ** -0.5, 0.125, ((1, 16), (2, 2)))
    w_out = noise(keys[5], (EXPERTS * HID, D), HID ** -0.5, 0.21875, ((0, 16), (1, 2)))
    grad_in = noise(keys[6], (N_DP, 2, EXPERTS * HID, D), 1.0, 6.0, ((0, 2), (2, 16)))
    grad_out = noise(keys[7], (N_DP, EXPERTS * HID, D), 1.0, 6.0, ((0, 2), (1, 16)))
    first_in = noise(keys[8], (2, EXPERTS * HID, D), 0.5, 3.0, ((1, 16), (2, 2)))
    second_in = jnp.clip(jnp.exp(math.log(4.0) - 2.7725887 * jax.random.uniform(keys[9], (2, EXPERTS * HID, D), jnp.float32) ** shard_levels(keys[9], (2, EXPERTS * HID, D), ((1, 16), (2, 2)), -0.2, 0.2)), 0.25, 4.0).astype(jnp.bfloat16)
    first_out = noise(keys[10], (EXPERTS * HID, D), 0.5, 3.0, ((0, 16), (1, 2)))
    second_out = jnp.clip(jnp.exp(math.log(4.0) - 2.7725887 * jax.random.uniform(keys[11], (EXPERTS * HID, D), jnp.float32) ** shard_levels(keys[11], (EXPERTS * HID, D), ((0, 16), (1, 2)), -0.2, 0.2)), 0.25, 4.0).astype(jnp.bfloat16)
    return dict(tokens=tokens, routes=routes, combine_weight=combine_weight, owner_plan=owner_plan, w_in=w_in, w_out=w_out, grad_in=grad_in, grad_out=grad_out, first_in=first_in, second_in=second_in, first_out=first_out, second_out=second_out)


BETA_ONE = 0.9
BETA_TWO = 0.95
LEARNING_RATE = 0.005
EPSILON = 1e-08
CORRECT_FIRST = 1.0 / (1.0 - 0.9 ** 10)
CORRECT_SECOND = 1.0 / (1.0 - 0.95 ** 10)

def adam_update(weight, gradient, first_moment, second_moment):
    first_next = BETA_ONE * first_moment.astype(jnp.float32) + (1.0 - BETA_ONE) * gradient
    second_next = BETA_TWO * second_moment.astype(jnp.float32) + (1.0 - BETA_TWO) * gradient * gradient
    stepped = weight.astype(jnp.float32) - LEARNING_RATE * (first_next * CORRECT_FIRST) / (jnp.sqrt(second_next * CORRECT_SECOND) + EPSILON)
    return (stepped.astype(jnp.bfloat16), first_next.astype(jnp.bfloat16), second_next.astype(jnp.bfloat16))

def slot_ranks(flat_routes):
    onehot = (flat_routes[:, None] == jnp.arange(EXPERTS, dtype=jnp.int32)[None, :]).astype(jnp.int32)
    ranks = jnp.cumsum(onehot, axis=0) - 1
    return lax.optimization_barrier(jnp.sum(ranks * onehot, axis=1)).astype(jnp.int32)

def times_rows(row_data, weight_rows):
    return lax.dot_general(row_data, weight_rows, (((1,), (1,)), ((), ())), preferred_element_type=jnp.float32)

def expert_rows(row_data, weight_in, weight_out):
    gate = times_rows(row_data, weight_in[0])
    upward = times_rows(row_data, weight_in[1])
    hidden = (jax.nn.silu(gate) * upward).astype(jnp.bfloat16)
    return jnp.dot(hidden, weight_out, preferred_element_type=jnp.float32).astype(jnp.bfloat16)

def expert_output(row_data, weight_in, weight_out):
    total = jnp.zeros((row_data.shape[0], weight_out.shape[1]), jnp.float32)
    for quarter in range(GROUP):
        begin = quarter * HDEV
        total = total + expert_rows(row_data, weight_in[:, begin:begin + HDEV], weight_out[begin:begin + HDEV]).astype(jnp.float32)
    return total.astype(jnp.bfloat16)

def reference(tokens, routes, combine_weight, owner_plan, w_in, w_out, grad_in, grad_out, first_in, second_in, first_out, second_out):
    width = tokens.shape[1]
    sum_in = lax.optimization_barrier(jnp.sum(grad_in.astype(jnp.float32), axis=0))
    sum_out = lax.optimization_barrier(jnp.sum(grad_out.astype(jnp.float32), axis=0))
    new_in, first_in_next, second_in_next = adam_update(w_in, sum_in, first_in, second_in)
    new_out, first_out_next, second_out_next = adam_update(w_out, sum_out, first_out, second_out)

    def regroup_in(moment):
        return jnp.take(moment.reshape(2, EXPERTS, HID, width), owner_plan, axis=1).reshape(moment.shape)

    def regroup_out(moment):
        return jnp.take(moment.reshape(EXPERTS, HID, width), owner_plan, axis=0).reshape(moment.shape)
    device_routes = routes.reshape(DEVICES, TOK_DEV * TOP)
    ranks = jax.vmap(slot_ranks)(device_routes)
    targets = (device_routes * CAP + ranks).astype(jnp.int32)
    token_ids = jnp.arange(TOKENS, dtype=jnp.int32).reshape(DEVICES, TOK_DEV)
    token_of_route = jnp.repeat(token_ids, TOP, axis=1)
    device_ids = jnp.repeat(jnp.arange(DEVICES, dtype=jnp.int32)[:, None], TOK_DEV * TOP, axis=1)
    table = jnp.zeros((DEVICES, EXPERTS * CAP), jnp.int32).at[device_ids, targets].set(token_of_route)
    weight_table = jnp.zeros((DEVICES, EXPERTS * CAP), jnp.float32).at[device_ids, targets].set(combine_weight.reshape(DEVICES, TOK_DEV * TOP))

    def one_expert(total, expert):
        start = (expert * CAP).astype(jnp.int32)
        row_ids = lax.dynamic_slice_in_dim(table, start, CAP, 1).reshape(-1)
        row_weights = lax.dynamic_slice_in_dim(weight_table, start, CAP, 1).reshape(-1)
        weight_in = lax.dynamic_slice_in_dim(new_in, (expert * HID).astype(jnp.int32), HID, 1)
        weight_out = lax.dynamic_slice_in_dim(new_out, (expert * HID).astype(jnp.int32), HID, 0)
        result = expert_output(tokens[row_ids], weight_in, weight_out)
        return (total.at[row_ids].add(row_weights[:, None] * result.astype(jnp.float32)), None)
    total, ignored = lax.scan(one_expert, jnp.zeros((TOKENS, width), jnp.float32), jnp.arange(EXPERTS, dtype=jnp.int32))
    return (total.astype(jnp.bfloat16), regroup_in(first_in_next), regroup_in(second_in_next), regroup_out(first_out_next), regroup_out(second_out_next))
```

```python
import functools

import jax
import jax.numpy as jnp
from jax import lax
from jax.experimental import pallas as pl
from jax.experimental.pallas import tpu as pltpu
from jax.sharding import PartitionSpec as P

GROUP = 4

BETA_ONE = 0.9
BETA_TWO = 0.95
LEARNING_RATE = 0.005
EPSILON = 1e-08
CORRECT_FIRST = 1.0 / (1.0 - 0.9**10)
CORRECT_SECOND = 1.0 / (1.0 - 0.95**10)

PLANES = 4
SPLITS = 2
TOKEN_SPLITS = 2
STRIP = 16
TILE = 256
MESH = pl.DeviceIdType.MESH


def adam_update(weight, gradient, first_moment, second_moment):
    first_next = BETA_ONE * first_moment.astype(jnp.float32) + (1.0 - BETA_ONE) * gradient
    second_next = (
        BETA_TWO * second_moment.astype(jnp.float32) + (1.0 - BETA_TWO) * gradient * gradient
    )
    stepped = weight.astype(jnp.float32) - LEARNING_RATE * (first_next * CORRECT_FIRST) / (
        jnp.sqrt(second_next * CORRECT_SECOND) + EPSILON
    )
    return (
        stepped.astype(jnp.bfloat16),
        first_next.astype(jnp.bfloat16),
        second_next.astype(jnp.bfloat16),
    )


def layer_kernel(
    mask,
    tokens,
    table,
    w_in,
    w_out,
    grad_in,
    grad_out,
    first_in,
    second_in,
    first_out,
    second_out,
    combined,
    first_in_next,
    second_in_next,
    first_out_next,
    second_out_next,
    rows_all,
    table_all,
    kept,
    came,
    old_weight,
    old_first,
    old_second,
    new_first,
    new_second,
    gathered,
    hidden,
    results,
    sums,
    scales,
    final,
    load_sem,
    grad_sem,
    y_sem,
    x_sem,
    core_sem,
    moment_sem,
    token_sem,
    table_sem,
    chain_sem,
    store_sem,
):
    token_count, width = tokens.shape
    half = width // 2
    hid = w_out.shape[0]
    quarters = gathered.shape[2] // hid
    chunk = hid // SPLITS
    chunks = 3 * SPLITS
    part = token_count // TOKEN_SPLITS

    e = lax.axis_index("expert")
    y = lax.axis_index("dp")
    z = lax.div(e, quarters)
    mine = lax.rem(e, quarters)
    core = lax.rem(e, 2)
    side = lax.div(mine, 2)
    core_e = e + 1 - 2 * core
    x_e = e + 2 - 4 * side
    low = lax.rem(z, 2)
    high = lax.div(z, 2)

    def flipped(bits):
        moved = e
        if bits & 1:
            moved = moved + quarters * (1 - 2 * low)
        if bits & 2:
            moved = moved + 2 * quarters * (1 - 2 * high)
        return moved

    def multiple(value, factor):
        return pl.multiple_of(value, factor)

    def remote(src, dst, sem, index, target):
        return pltpu.make_async_remote_copy(
            src_ref=src,
            dst_ref=dst,
            send_sem=sem.at[(0,) + index],
            recv_sem=sem.at[(1,) + index],
            device_id=target,
            device_id_type=MESH,
        )

    def shard(pair, single, m):
        return pair.at[m] if m < 2 else single

    def gradient(m):
        return grad_in.at[0, m] if m < 2 else grad_out.at[0]

    stays = pl.ds(multiple(y * half, 128), half)
    leaves = pl.ds(multiple((1 - y) * half, 128), half)
    loads = []
    for m in range(3):
        block = pl.ds(m * hid, hid)
        loads.append(
            [
                pltpu.make_async_copy(src, dst.at[block], load_sem.at[4 * m + i])
                for i, (src, dst) in enumerate(
                    (
                        (gradient(m).at[:, stays], kept),
                        (shard(first_in, first_out, m), old_first),
                        (shard(second_in, second_out, m), old_second),
                        (shard(w_in, w_out, m), old_weight),
                    )
                )
            ]
        )
    own_rows = pl.ds(multiple(z * token_count, token_count), token_count)
    small = [
        pltpu.make_async_copy(tokens, rows_all.at[own_rows], load_sem.at[12]),
        pltpu.make_async_copy(table, table_all.at[z], load_sem.at[13]),
    ]
    for m in range(3):
        for load in loads[m]:
            load.start()
    for load in small:
        load.start()

    barrier = pltpu.get_barrier_semaphore()
    for target in (
        (core_e, y),
        (x_e, y),
        (e, 1 - y),
        (flipped(1), y),
        (flipped(2), y),
        (flipped(3), y),
    ):
        pl.semaphore_signal(barrier, inc=1, device_id=target, device_id_type=MESH)
    pl.semaphore_wait(barrier, 6)

    def grad_copy(k):
        m, r = divmod(k, SPLITS)
        return remote(
            gradient(m).at[pl.ds(r * chunk, chunk), leaves],
            came.at[pl.ds(k * chunk, chunk)],
            grad_sem,
            (k,),
            (e, 1 - y),
        )

    def token_copy(direction, hop, c):
        plane = z + hop if direction == 0 else z - hop
        there = pl.ds(multiple(plane * token_count + c * part, part), part)
        src = tokens.at[pl.ds(c * part, part)] if hop == 0 else rows_all.at[there]
        target = e - quarters if direction == 0 else e + quarters
        return remote(src, rows_all.at[there], token_sem, (direction, hop, c), (target, y))

    def token_sends(direction, hop):
        if direction == 0:
            return jnp.logical_and(z > 0, z + hop <= PLANES - 1)
        return jnp.logical_and(z < PLANES - 1, z - hop >= 0)

    def token_arrives(direction, hop):
        return z + 1 + hop <= PLANES - 1 if direction == 0 else z - 1 - hop >= 0

    def relay_tokens(hop, c):
        for direction in range(2):

            @pl.when(token_arrives(direction, hop - 1))
            def _():
                token_copy(direction, hop - 1, c).wait_recv()

            if hop < PLANES - 1:

                @pl.when(token_sends(direction, hop))
                def _():
                    token_copy(direction, hop, c).start()

    table_copies = [
        remote(table, table_all.at[z], table_sem, (bits - 1,), (flipped(bits), y))
        for bits in range(1, PLANES)
    ]

    for k in range(chunks):
        grad_copy(k).start()
    for c in range(TOKEN_SPLITS):
        for direction in range(2):

            @pl.when(token_sends(direction, 0))
            def _():
                token_copy(direction, 0, c).start()

    for copy in table_copies:
        copy.start()

    def weight_block(k, width_half, quarter):
        m, r = divmod(k, SPLITS)
        return gathered.at[
            m, width_half, pl.ds(multiple(quarter * hid + r * chunk, chunk), chunk)
        ]

    x_quarter = mine + 2 - 4 * side
    sources = ((y, mine), (1 - y, mine), (y, x_quarter), (1 - y, x_quarter))

    def y_copy(k):
        block = weight_block(k, y, mine)
        return remote(block, block, y_sem, (k,), (e, 1 - y))

    def x_copy(j, k):
        block = weight_block(k, *sources[j])
        return remote(block, block, x_sem, (j, k), (x_e, y))

    def core_copy(j, k):
        block = weight_block(k, *sources[j])
        return remote(block, block, core_sem, (j, k), (core_e, y))

    def moment_copies(k):
        m, r = divmod(k, SPLITS)
        here, there = pl.ds(k * chunk, chunk), pl.ds(r * chunk, chunk)
        return [
            remote(
                new.at[here],
                shard(pair, single, m).at[there],
                moment_sem,
                (i, k),
                (flipped(mask), y),
            )
            for i, (new, pair, single) in enumerate(
                (
                    (new_first, first_in_next, first_out_next),
                    (new_second, second_in_next, second_out_next),
                )
            )
        ]

    at_once = chunks if mask == 1 else (2 * chunks) // 3

    for k in range(chunks):
        m, r = divmod(k, SPLITS)
        if r == 0:
            for load in loads[m]:
                load.wait()
        grad_copy(k).wait_recv()

        @pl.loop(0, chunk // STRIP)
        def _(i):
            at = pl.ds(multiple(k * chunk + i * STRIP, STRIP), STRIP)
            total = kept[at, :].astype(jnp.float32) + came[at, :].astype(jnp.float32)
            weight, first, second = adam_update(
                old_weight[at, :], total, old_first[at, :], old_second[at, :]
            )
            place = pl.ds(multiple(mine * hid + r * chunk + i * STRIP, STRIP), STRIP)
            gathered[m, y, place, :] = weight
            new_first[at, :] = first
            new_second[at, :] = second

        x_copy(0, k).start()
        y_copy(k).start()
        core_copy(0, k).start()
        if k < at_once:
            for copy in moment_copies(k):
                copy.start()
        if 1 <= k < 1 + TOKEN_SPLITS:
            relay_tokens(1, k - 1)
        if 2 + TOKEN_SPLITS <= k < 2 + 2 * TOKEN_SPLITS:
            relay_tokens(2, k - 2 - TOKEN_SPLITS)

    for k in range(chunks):
        y_copy(k).wait_recv()
        x_copy(1, k).start()
        core_copy(1, k).start()
        x_copy(0, k).wait_recv()
        core_copy(2, k).start()
    for c in range(TOKEN_SPLITS):
        relay_tokens(3, c)

    for load in small:
        load.wait()
    for copy in table_copies:
        copy.wait_recv()
    diagonal = lax.broadcasted_iota(jnp.int32, (token_count, token_count), 0) == (
        lax.broadcasted_iota(jnp.int32, (token_count, token_count), 1)
    )
    for plane in range(PLANES):
        line = table_all[plane, pl.ds(z, 1), :]
        column = jnp.sum(jnp.where(diagonal, line, 0.0), axis=1, keepdims=True)
        scales[pl.ds(plane * token_count, token_count), :] = jnp.broadcast_to(
            column, (token_count, scales.shape[1])
        )

    for k in range(chunks):
        x_copy(1, k).wait_recv()
        core_copy(3, k).start()
    for k in range(chunks):
        for j in range(4):
            core_copy(j, k).wait_recv()

    row_tiles = rows_all.shape[0] // TILE
    contract = (((1,), (1,)), ((), ()))

    @pl.loop(0, (quarters * hid // TILE) * row_tiles)
    def _(t):
        at = pl.ds(multiple(lax.rem(t, row_tiles) * TILE, TILE), TILE)
        units = pl.ds(multiple(lax.div(t, row_tiles) * TILE, TILE), TILE)

        def times_rows(m):
            return sum(
                lax.dot_general(
                    rows_all[at, s * half : (s + 1) * half],
                    gathered[m, s, units, :],
                    contract,
                    preferred_element_type=jnp.float32,
                )
                for s in range(2)
            )

        gate, upward = times_rows(0), times_rows(1)
        hidden[at, units] = (jax.nn.silu(gate) * upward).astype(jnp.bfloat16)

    for s in range(2):

        @pl.loop(0, (half // TILE) * row_tiles)
        def _(t):
            at = pl.ds(multiple(lax.rem(t, row_tiles) * TILE, TILE), TILE)
            from_column = lax.div(t, row_tiles) * TILE
            results[at, pl.ds(multiple(s * half + from_column, TILE), TILE)] = jnp.dot(
                hidden[at, :],
                gathered[2, s, :, pl.ds(multiple(from_column, TILE), TILE)],
                preferred_element_type=jnp.float32,
            ).astype(jnp.bfloat16)

    inner = jnp.logical_and(z > 0, z < PLANES - 1)

    def held_moments():
        for k in range(at_once, chunks):
            for copy in moment_copies(k):
                copy.start()

    if at_once < chunks:
        pl.when(inner)(held_moments)

    def chain_copy(direction, i, c):
        plane = i + direction * (PLANES - 1 - 2 * i)
        at = pl.ds(multiple(plane * token_count + c * part, part), part)
        target = e + quarters * (2 * direction - 1)
        return remote(
            results.at[at], sums.at[direction, at], chain_sem, (direction, i, c), (target, y)
        )

    def chain_step(t, act):
        i = lax.div(t, 2 * TOKEN_SPLITS)
        c = lax.rem(lax.div(t, 2), TOKEN_SPLITS)
        direction = lax.rem(t + 1 - high, 2)
        depth = z + direction * (PLANES - 1 - 2 * z)
        act(direction, i, c, depth)

    def send_sums(direction, i, c, depth):
        @pl.when(depth > i)
        def _():
            copy = chain_copy(direction, i, c)

            @pl.when(depth < PLANES - 1)
            def _():
                copy.wait_recv()

            plane = i + direction * (PLANES - 1 - 2 * i)

            @pl.loop(0, part // STRIP)
            def _(s):
                at = pl.ds(
                    multiple(plane * token_count + c * part + s * STRIP, STRIP), STRIP
                )
                value = results[at, :].astype(jnp.float32) * scales[at, 0:1]
                before = sums[direction, at, :].astype(jnp.float32)
                results[at, :] = (
                    value + jnp.where(depth < PLANES - 1, before, 0.0)
                ).astype(jnp.bfloat16)

            copy.start()

    def drain_sums(direction, i, c, depth):
        @pl.when(depth > i)
        def _():
            chain_copy(direction, i, c).wait_send()

    steps = 2 * TOKEN_SPLITS * (PLANES - 1)

    @pl.loop(0, steps)
    def _(t):
        chain_step(t, send_sums)

    if at_once < chunks:
        pl.when(jnp.logical_not(inner))(held_moments)

    for c in range(TOKEN_SPLITS):

        @pl.when(z < PLANES - 1)
        def _():
            chain_copy(0, z, c).wait_recv()

        @pl.when(z > 0)
        def _():
            chain_copy(1, PLANES - 1 - z, c).wait_recv()

        @pl.loop(0, part // STRIP)
        def _(s):
            at = pl.ds(multiple(z * token_count + c * part + s * STRIP, STRIP), STRIP)
            value = results[at, :].astype(jnp.float32) * scales[at, 0:1]
            above = sums[0, at, :].astype(jnp.float32)
            below = sums[1, at, :].astype(jnp.float32)
            value = value + jnp.where(z < PLANES - 1, above, 0.0)
            value = value + jnp.where(z > 0, below, 0.0)
            final[pl.ds(multiple(c * part + s * STRIP, STRIP), STRIP), :] = value.astype(
                jnp.bfloat16
            )

    store = pltpu.make_async_copy(final, combined, store_sem.at[0])
    store.start()

    for k in range(chunks):
        grad_copy(k).wait_send()
        y_copy(k).wait_send()
        for j in range(2):
            x_copy(j, k).wait_send()
        for j in range(4):
            core_copy(j, k).wait_send()
        for copy in moment_copies(k):
            copy.wait_send()
            copy.wait_recv()
    for c in range(TOKEN_SPLITS):
        for hop in range(PLANES - 1):
            for direction in range(2):

                @pl.when(token_sends(direction, hop))
                def _():
                    token_copy(direction, hop, c).wait_send()

    for copy in table_copies:
        copy.wait_send()

    @pl.loop(0, steps)
    def _(t):
        chain_step(t, drain_sums)

    store.wait()


def layer_call(
    mask,
    tokens,
    routes,
    combine_weight,
    w_in,
    w_out,
    grad_in,
    grad_out,
    first_in,
    second_in,
    first_out,
    second_out,
):
    token_count, width = tokens.shape
    half = width // 2
    hid = w_out.shape[0]
    lanes = 128
    experts = jnp.arange(8, dtype=jnp.int32)
    table = jnp.sum(
        jnp.where(
            routes.T[:, None, :] == experts[None, :, None], combine_weight.T[:, None, :], 0.0
        ),
        axis=0,
    )
    any_space = pl.BlockSpec(memory_space=pl.ANY)
    bf16, dma = jnp.bfloat16, pltpu.SemaphoreType.DMA
    chunks = 3 * SPLITS
    outs = (tokens, first_in, second_in, first_out, second_out)
    rows = PLANES * token_count
    return pl.pallas_call(
        functools.partial(layer_kernel, mask),
        name=f"layer_{mask}",
        out_shape=tuple(jax.ShapeDtypeStruct(out.shape, out.dtype) for out in outs),
        in_specs=[any_space] * 10,
        out_specs=(any_space,) * 5,
        scratch_shapes=[
            pltpu.VMEM((rows, width), bf16),
            pltpu.VMEM((PLANES, 8, token_count), jnp.float32),
            pltpu.VMEM((3 * hid, half), bf16),
            pltpu.VMEM((3 * hid, half), bf16),
            pltpu.VMEM((3 * hid, half), bf16),
            pltpu.VMEM((3 * hid, half), bf16),
            pltpu.VMEM((3 * hid, half), bf16),
            pltpu.VMEM((3 * hid, half), bf16),
            pltpu.VMEM((3 * hid, half), bf16),
            pltpu.VMEM((3, 2, GROUP * hid, half), bf16),
            pltpu.VMEM((rows, GROUP * hid), bf16),
            pltpu.VMEM((rows, width), bf16),
            pltpu.VMEM((2, rows, width), bf16),
            pltpu.VMEM((rows, lanes), jnp.float32),
            pltpu.VMEM((token_count, width), bf16),
            dma((14,)),
            dma((2, chunks)),
            dma((2, chunks)),
            dma((2, 2, chunks)),
            dma((2, 4, chunks)),
            dma((2, 2, chunks)),
            dma((2, 2, PLANES - 1, TOKEN_SPLITS)),
            dma((2, PLANES - 1)),
            dma((2, 2, PLANES - 1, TOKEN_SPLITS)),
            dma((1,)),
        ],
        compiler_params=pltpu.CompilerParams(
            collective_id=mask, has_side_effects=True, vmem_limit_bytes=60 * 1024 * 1024
        ),
    )(
        tokens,
        table,
        w_in,
        w_out,
        grad_in,
        grad_out,
        first_in,
        second_in,
        first_out,
        second_out,
    )


def exchanged(block, axis, mask):
    return lax.ppermute(block, axis, [(i, i ^ mask) for i in range(lax.axis_size(axis))])


def slot_ranks(flat_routes, expert_count):
    onehot = (flat_routes[:, None] == jnp.arange(expert_count, dtype=jnp.int32)[None, :]).astype(
        jnp.int32
    )
    ranks = jnp.cumsum(onehot, axis=0) - 1
    return jnp.sum(ranks * onehot, axis=1)


def times_rows(row_data, weight_rows):
    return lax.dot_general(
        row_data, weight_rows, (((1,), (1,)), ((), ())), preferred_element_type=jnp.float32
    )


def migrate_any(moment, source_rows, device_count):
    spread = lax.all_to_all(
        moment.reshape(device_count, -1), "expert", split_axis=0, concat_axis=0, tiled=True
    )
    picked = jnp.take(spread, source_rows, axis=0)
    landed = lax.all_to_all(picked, "expert", split_axis=0, concat_axis=0, tiled=True)
    return landed.reshape(moment.shape)


def summed_half(gradient, dp_index):
    half = gradient.shape[1] // 2
    kept = lax.dynamic_slice_in_dim(gradient, dp_index * half, half, 1)
    leaving = lax.dynamic_slice_in_dim(gradient, (1 - dp_index) * half, half, 1)
    return kept.astype(jnp.float32) + exchanged(leaving, "dp", 1).astype(jnp.float32)


def gathered(piece):
    pieces = {(0, 0): piece, (0, 1): exchanged(piece, "dp", 1)}
    for side in range(2):
        pieces[2, side] = exchanged(pieces[0, side], "expert", 2)
    for side in range(2):
        pieces[1, side] = exchanged(pieces[0, side], "expert", 1)
        pieces[3, side] = exchanged(pieces[2, side], "expert", 1)
    return pieces


def body(
    move,
    tokens,
    routes,
    combine_weight,
    w_in,
    w_out,
    grad_in,
    grad_out,
    first_in,
    second_in,
    first_out,
    second_out,
):
    device_count = lax.axis_size("expert")
    expert_count = device_count // GROUP
    token_count, route_count = routes.shape
    width = tokens.shape[1]
    half = width // 2
    capacity = GROUP * (
        (token_count * route_count * 4 + 3 * expert_count * GROUP - 1) // (3 * expert_count * GROUP)
    )
    dp_index = lax.axis_index("dp")
    my_group = lax.axis_index("expert") // GROUP

    flat_routes = routes.reshape(-1)
    ranks = slot_ranks(flat_routes, expert_count)
    relative = flat_routes ^ my_group
    targets = (relative * capacity + ranks).reshape(token_count, route_count)
    slot_ids = jnp.arange(expert_count * capacity, dtype=jnp.int32)
    selector = jnp.any(targets[None, :, :] == slot_ids[:, None, None], axis=2).astype(jnp.bfloat16)
    outgoing = jnp.dot(selector, tokens, preferred_element_type=jnp.float32).astype(jnp.bfloat16)
    outgoing = outgoing.reshape(expert_count, capacity, width)
    arrived = [outgoing[0]] + [
        exchanged(outgoing[mask], "expert", mask * GROUP) for mask in range(1, expert_count)
    ]

    weights = (w_in[0], w_in[1], w_out)
    gradients = (grad_in[0, 0], grad_in[0, 1], grad_out[0])
    firsts = (first_in[0], first_in[1], first_out)
    seconds = (second_in[0], second_in[1], second_out)
    sums = [summed_half(gradient, dp_index) for gradient in gradients]
    stepped = [adam_update(*arrays) for arrays in zip(weights, sums, firsts, seconds)]
    gate_pieces, up_pieces, out_pieces = [gathered(step[0]) for step in stepped]
    moved_first = [move(step[1]) for step in stepped]
    moved_second = [move(step[2]) for step in stepped]

    rows = jnp.concatenate(arrived, 0)
    sides = [
        lax.dynamic_slice_in_dim(rows, dp_index * half, half, 1),
        lax.dynamic_slice_in_dim(rows, (1 - dp_index) * half, half, 1),
    ]
    totals = [jnp.zeros((rows.shape[0], half), jnp.float32) for _ in range(2)]
    for quarter in (0, 1, 2, 3):
        gate = times_rows(sides[0], gate_pieces[quarter, 0]) + times_rows(
            sides[1], gate_pieces[quarter, 1]
        )
        upward = times_rows(sides[0], up_pieces[quarter, 0]) + times_rows(
            sides[1], up_pieces[quarter, 1]
        )
        hidden = (jax.nn.silu(gate) * upward).astype(jnp.bfloat16)
        for side in range(2):
            part = jnp.dot(
                hidden, out_pieces[quarter, side], preferred_element_type=jnp.float32
            ).astype(jnp.bfloat16)
            totals[side] = totals[side] + part.astype(jnp.float32)
    near, far = [total.astype(jnp.bfloat16) for total in totals]
    results = jnp.where(
        dp_index == 0, jnp.concatenate([near, far], 1), jnp.concatenate([far, near], 1)
    ).reshape(expert_count, capacity, width)
    returned = [results[0]] + [
        exchanged(results[mask], "expert", mask * GROUP) for mask in range(1, expert_count)
    ]
    by_slot = jnp.concatenate(returned, 0)
    weight_table = jnp.sum(
        jnp.where(targets[:, :, None] == slot_ids[None, None, :], combine_weight[:, :, None], 0.0),
        axis=1,
    )
    weight_high = weight_table.astype(jnp.bfloat16)
    weight_low = (weight_table - weight_high.astype(jnp.float32)).astype(jnp.bfloat16)
    combined = (
        jnp.dot(weight_high, by_slot, preferred_element_type=jnp.float32)
        + jnp.dot(weight_low, by_slot, preferred_element_type=jnp.float32)
    ).astype(jnp.bfloat16)
    return (
        combined,
        jnp.stack(moved_first[:2]),
        jnp.stack(moved_second[:2]),
        moved_first[2],
        moved_second[2],
    )


def local(tokens, routes, combine_weight, owner_plan, *state):
    device_count = lax.axis_size("expert")
    expert_count = device_count // GROUP
    operands = (tokens, routes, combine_weight) + state
    if expert_count == PLANES and lax.axis_size("dp") == 2:
        branches = [functools.partial(layer_call, mask) for mask in range(1, expert_count)]
        return lax.switch(owner_plan[0] - 1, branches, *operands)
    device_ids = jnp.arange(device_count, dtype=jnp.int32)
    source_rows = jnp.take(owner_plan, device_ids // GROUP) * GROUP + device_ids % GROUP
    return body(lambda moment: migrate_any(moment, source_rows, device_count), *operands)


def solution(mesh):
    in_specs = (
        P(("expert", "dp"), None),
        P(("expert", "dp"), None),
        P(("expert", "dp"), None),
        P(),
        P(None, "expert", "dp"),
        P("expert", "dp"),
        P("dp", None, "expert", None),
        P("dp", "expert", None),
        P(None, "expert", "dp"),
        P(None, "expert", "dp"),
        P("expert", "dp"),
        P("expert", "dp"),
    )
    out_specs = (
        P(("expert", "dp"), None),
        P(None, "expert", "dp"),
        P(None, "expert", "dp"),
        P("expert", "dp"),
        P("expert", "dp"),
    )
    return jax.shard_map(local, mesh=mesh, in_specs=in_specs, out_specs=out_specs, check_vma=False)
```

```python
import functools

import jax
import jax.numpy as jnp
from jax import lax
from jax.experimental import pallas as pl
from jax.experimental.pallas import tpu as pltpu
from jax.sharding import PartitionSpec as P

GROUP = 4

BETA_ONE = 0.9
BETA_TWO = 0.95
LEARNING_RATE = 0.005
EPSILON = 1e-08
CORRECT_FIRST = 1.0 / (1.0 - 0.9**10)
CORRECT_SECOND = 1.0 / (1.0 - 0.95**10)

PLANES = 4
SPLITS = 2
TOKEN_SPLITS = 2
STRIP = 16
TILE = 256
MESH = pl.DeviceIdType.MESH


def adam_update(weight, gradient, first_moment, second_moment):
    first_next = BETA_ONE * first_moment.astype(jnp.float32) + (1.0 - BETA_ONE) * gradient
    second_next = (
        BETA_TWO * second_moment.astype(jnp.float32) + (1.0 - BETA_TWO) * gradient * gradient
    )
    stepped = weight.astype(jnp.float32) - LEARNING_RATE * (first_next * CORRECT_FIRST) / (
        jnp.sqrt(second_next * CORRECT_SECOND) + EPSILON
    )
    return (
        stepped.astype(jnp.bfloat16),
        first_next.astype(jnp.bfloat16),
        second_next.astype(jnp.bfloat16),
    )


def layer_kernel(
    mask,
    tokens,
    routes,
    combine_weight,
    w_in,
    w_out,
    grad_in,
    grad_out,
    first_in,
    second_in,
    first_out,
    second_out,
    combined,
    first_in_next,
    second_in_next,
    first_out_next,
    second_out_next,
    rows_all,
    own_routes,
    own_weights,
    table_all,
    kept,
    came,
    old_weight,
    old_first,
    old_second,
    new_first,
    new_second,
    gathered,
    hidden,
    results,
    sums,
    scales,
    final,
    load_sem,
    grad_sem,
    y_sem,
    x_sem,
    core_sem,
    moment_sem,
    token_sem,
    table_sem,
    chain_sem,
    store_sem,
):
    token_count, width = tokens.shape
    half = width // 2
    hid = w_out.shape[0]
    quarters = gathered.shape[2] // hid
    chunk = hid // SPLITS
    chunks = 3 * SPLITS
    part = token_count // TOKEN_SPLITS

    e = lax.axis_index("expert")
    y = lax.axis_index("dp")
    z = lax.div(e, quarters)
    mine = lax.rem(e, quarters)
    core = lax.rem(e, 2)
    side = lax.div(mine, 2)
    core_e = e + 1 - 2 * core
    x_e = e + 2 - 4 * side
    low = lax.rem(z, 2)
    high = lax.div(z, 2)

    def flipped(bits):
        moved = e
        if bits & 1:
            moved = moved + quarters * (1 - 2 * low)
        if bits & 2:
            moved = moved + 2 * quarters * (1 - 2 * high)
        return moved

    def multiple(value, factor):
        return pl.multiple_of(value, factor)

    def remote(src, dst, sem, index, target):
        return pltpu.make_async_remote_copy(
            src_ref=src,
            dst_ref=dst,
            send_sem=sem.at[(0,) + index],
            recv_sem=sem.at[(1,) + index],
            device_id=target,
            device_id_type=MESH,
        )

    def shard(pair, single, m):
        return pair.at[m] if m < 2 else single

    def gradient(m):
        return grad_in.at[0, m] if m < 2 else grad_out.at[0]

    stays = pl.ds(multiple(y * half, 128), half)
    leaves = pl.ds(multiple((1 - y) * half, 128), half)
    loads = []
    for m in range(3):
        block = pl.ds(m * hid, hid)
        loads.append(
            [
                pltpu.make_async_copy(src, dst.at[block], load_sem.at[4 * m + i])
                for i, (src, dst) in enumerate(
                    (
                        (gradient(m).at[:, stays], kept),
                        (shard(first_in, first_out, m), old_first),
                        (shard(second_in, second_out, m), old_second),
                        (shard(w_in, w_out, m), old_weight),
                    )
                )
            ]
        )
    own_rows = pl.ds(multiple(z * token_count, token_count), token_count)
    small = [
        pltpu.make_async_copy(tokens, rows_all.at[own_rows], load_sem.at[12]),
        pltpu.make_async_copy(routes, own_routes, load_sem.at[13]),
        pltpu.make_async_copy(combine_weight, own_weights, load_sem.at[14]),
    ]
    for m in range(3):
        for load in loads[m]:
            load.start()
    for load in small:
        load.start()

    barrier = pltpu.get_barrier_semaphore()
    for target in (
        (core_e, y),
        (x_e, y),
        (e, 1 - y),
        (flipped(1), y),
        (flipped(2), y),
        (flipped(3), y),
    ):
        pl.semaphore_signal(barrier, inc=1, device_id=target, device_id_type=MESH)
    pl.semaphore_wait(barrier, 6)

    def grad_copy(k):
        m, r = divmod(k, SPLITS)
        return remote(
            gradient(m).at[pl.ds(r * chunk, chunk), leaves],
            came.at[pl.ds(k * chunk, chunk)],
            grad_sem,
            (k,),
            (e, 1 - y),
        )

    def token_copy(direction, hop, c):
        plane = z + hop if direction == 0 else z - hop
        there = pl.ds(multiple(plane * token_count + c * part, part), part)
        src = tokens.at[pl.ds(c * part, part)] if hop == 0 else rows_all.at[there]
        target = e - quarters if direction == 0 else e + quarters
        return remote(src, rows_all.at[there], token_sem, (direction, hop, c), (target, y))

    def token_sends(direction, hop):
        if direction == 0:
            return jnp.logical_and(z > 0, z + hop <= PLANES - 1)
        return jnp.logical_and(z < PLANES - 1, z - hop >= 0)

    def token_arrives(direction, hop):
        return z + 1 + hop <= PLANES - 1 if direction == 0 else z - 1 - hop >= 0

    def relay_tokens(hop, c):
        for direction in range(2):

            @pl.when(token_arrives(direction, hop - 1))
            def _():
                token_copy(direction, hop - 1, c).wait_recv()

            if hop < PLANES - 1:

                @pl.when(token_sends(direction, hop))
                def _():
                    token_copy(direction, hop, c).start()

    table_copies = [
        remote(table_all.at[z], table_all.at[z], table_sem, (bits - 1,), (flipped(bits), y))
        for bits in range(1, PLANES)
    ]

    for k in range(chunks):
        grad_copy(k).start()
    for c in range(TOKEN_SPLITS):
        for direction in range(2):

            @pl.when(token_sends(direction, 0))
            def _():
                token_copy(direction, 0, c).start()

    for load in small:
        load.wait()
    experts = lax.broadcasted_iota(jnp.int32, table_all.shape[1:], 0)
    table = jnp.zeros(table_all.shape[1:], jnp.float32)
    for route in range(own_routes.shape[0]):
        named = experts == own_routes[route : route + 1, :]
        table = table + jnp.where(named, own_weights[route : route + 1, :], 0.0)
    table_all[z] = table

    def weight_block(k, width_half, quarter):
        m, r = divmod(k, SPLITS)
        return gathered.at[
            m, width_half, pl.ds(multiple(quarter * hid + r * chunk, chunk), chunk)
        ]

    x_quarter = mine + 2 - 4 * side
    sources = ((y, mine), (1 - y, mine), (y, x_quarter), (1 - y, x_quarter))

    def y_copy(k):
        block = weight_block(k, y, mine)
        return remote(block, block, y_sem, (k,), (e, 1 - y))

    def x_copy(j, k):
        block = weight_block(k, *sources[j])
        return remote(block, block, x_sem, (j, k), (x_e, y))

    def core_copy(j, k):
        block = weight_block(k, *sources[j])
        return remote(block, block, core_sem, (j, k), (core_e, y))

    def moment_copies(k):
        m, r = divmod(k, SPLITS)
        here, there = pl.ds(k * chunk, chunk), pl.ds(r * chunk, chunk)
        return [
            remote(
                new.at[here],
                shard(pair, single, m).at[there],
                moment_sem,
                (i, k),
                (flipped(mask), y),
            )
            for i, (new, pair, single) in enumerate(
                (
                    (new_first, first_in_next, first_out_next),
                    (new_second, second_in_next, second_out_next),
                )
            )
        ]

    inner = jnp.logical_and(z > 0, z < PLANES - 1)
    outer = jnp.logical_not(inner)
    inner_first = chunks if mask == 1 else (2 * chunks) // 3
    outer_first = chunks if mask == 1 else chunks // 2

    def send_moments(which, start, stop):
        @pl.when(which)
        def _():
            for k in range(start, stop):
                for copy in moment_copies(k):
                    copy.start()

    for k in range(chunks):
        m, r = divmod(k, SPLITS)
        if r == 0:
            for load in loads[m]:
                load.wait()
        grad_copy(k).wait_recv()

        @pl.loop(0, chunk // STRIP)
        def _(i):
            at = pl.ds(multiple(k * chunk + i * STRIP, STRIP), STRIP)
            total = kept[at, :].astype(jnp.float32) + came[at, :].astype(jnp.float32)
            weight, first, second = adam_update(
                old_weight[at, :], total, old_first[at, :], old_second[at, :]
            )
            place = pl.ds(multiple(mine * hid + r * chunk + i * STRIP, STRIP), STRIP)
            gathered[m, y, place, :] = weight
            new_first[at, :] = first
            new_second[at, :] = second

        x_copy(0, k).start()
        y_copy(k).start()
        core_copy(0, k).start()
        if mask == 1:
            send_moments(outer, k, k + 1)
        if k == 0:
            for copy in table_copies:
                copy.start()
        if k == 1:
            relay_tokens(1, 0)
        if k == 2:
            relay_tokens(1, 1)
        if k == 3:
            relay_tokens(2, 0)
        if k == 5:
            relay_tokens(2, 1)
        if mask == 1 and k == 5:
            send_moments(inner, 0, inner_first)
        if mask != 1 and k == 2:
            send_moments(inner, 0, 3)
        if mask != 1 and k > 2:
            send_moments(inner, k, min(k + 1, inner_first))

    for k in range(chunks):
        y_copy(k).wait_recv()
        x_copy(1, k).start()
        core_copy(1, k).start()
        x_copy(0, k).wait_recv()
        core_copy(2, k).start()
        if mask != 1 and k == 0:
            send_moments(outer, 0, outer_first)
    for c in range(TOKEN_SPLITS):
        relay_tokens(3, c)

    for copy in table_copies:
        copy.wait_recv()
    diagonal = lax.broadcasted_iota(jnp.int32, (token_count, token_count), 0) == (
        lax.broadcasted_iota(jnp.int32, (token_count, token_count), 1)
    )
    for plane in range(PLANES):
        line = table_all[plane, pl.ds(z, 1), :]
        column = jnp.sum(jnp.where(diagonal, line, 0.0), axis=1, keepdims=True)
        scales[pl.ds(plane * token_count, token_count), :] = jnp.broadcast_to(
            column, (token_count, scales.shape[1])
        )

    wide = 2 * SPLITS
    for k in range(wide):
        x_copy(1, k).wait_recv()
        core_copy(3, k).start()
    for k in range(wide):
        for j in range(4):
            core_copy(j, k).wait_recv()

    row_tiles = rows_all.shape[0] // TILE
    contract = (((1,), (1,)), ((), ()))

    @pl.loop(0, (quarters * hid // TILE) * row_tiles)
    def _(t):
        at = pl.ds(multiple(lax.rem(t, row_tiles) * TILE, TILE), TILE)
        units = pl.ds(multiple(lax.div(t, row_tiles) * TILE, TILE), TILE)

        def times_rows(m):
            return sum(
                lax.dot_general(
                    rows_all[at, s * half : (s + 1) * half],
                    gathered[m, s, units, :],
                    contract,
                    preferred_element_type=jnp.float32,
                )
                for s in range(2)
            )

        gate, upward = times_rows(0), times_rows(1)
        hidden[at, units] = (jax.nn.silu(gate) * upward).astype(jnp.bfloat16)

    def times_out(s):
        @pl.loop(0, (half // TILE) * row_tiles)
        def _(t):
            at = pl.ds(multiple(lax.rem(t, row_tiles) * TILE, TILE), TILE)
            from_column = lax.div(t, row_tiles) * TILE
            results[at, pl.ds(multiple(s * half + from_column, TILE), TILE)] = jnp.dot(
                hidden[at, :],
                gathered[2, s, :, pl.ds(multiple(from_column, TILE), TILE)],
                preferred_element_type=jnp.float32,
            ).astype(jnp.bfloat16)

    for k in range(wide, chunks):
        for j in (0, 2):
            core_copy(j, k).wait_recv()
    times_out(y)
    for k in range(wide, chunks):
        x_copy(1, k).wait_recv()
        core_copy(3, k).start()
    for k in range(wide, chunks):
        for j in (1, 3):
            core_copy(j, k).wait_recv()
    times_out(1 - y)

    def chain_copy(direction, i, c):
        plane = i + direction * (PLANES - 1 - 2 * i)
        at = pl.ds(multiple(plane * token_count + c * part, part), part)
        target = e + quarters * (2 * direction - 1)
        return remote(
            results.at[at], sums.at[direction, at], chain_sem, (direction, i, c), (target, y)
        )

    def chain_step(second, i, c, act):
        direction = high * second + (1 - high) * (1 - second)
        act(direction, i, c, z + direction * (PLANES - 1 - 2 * z))

    def chain_steps(second, act):
        @pl.loop(0, TOKEN_SPLITS * (PLANES - 1))
        def _(t):
            chain_step(second, lax.div(t, TOKEN_SPLITS), lax.rem(t, TOKEN_SPLITS), act)

    def send_sums(direction, i, c, depth):
        @pl.when(depth > i)
        def _():
            copy = chain_copy(direction, i, c)

            @pl.when(depth < PLANES - 1)
            def _():
                copy.wait_recv()

            plane = i + direction * (PLANES - 1 - 2 * i)

            @pl.loop(0, part // STRIP)
            def _(s):
                at = pl.ds(
                    multiple(plane * token_count + c * part + s * STRIP, STRIP), STRIP
                )
                value = results[at, :].astype(jnp.float32) * scales[at, 0:1]
                before = sums[direction, at, :].astype(jnp.float32)
                results[at, :] = (
                    value + jnp.where(depth < PLANES - 1, before, 0.0)
                ).astype(jnp.bfloat16)

            copy.start()

    def drain_sums(direction, i, c, depth):
        @pl.when(depth > i)
        def _():
            chain_copy(direction, i, c).wait_send()

    if mask == 1:
        for i in range(PLANES - 1):
            for c in range(TOKEN_SPLITS):
                chain_step(0, i, c, send_sums)
                late = i * TOKEN_SPLITS + c - 1
                if 0 <= late < TOKEN_SPLITS:
                    chain_step(1, 0, late, send_sums)
    else:
        chain_steps(0, send_sums)
        send_moments(outer, outer_first, chunks)
        send_moments(inner, inner_first, chunks)
        chain_steps(1, send_sums)

    for c in range(TOKEN_SPLITS):

        @pl.when(z < PLANES - 1)
        def _():
            chain_copy(0, z, c).wait_recv()

        @pl.when(z > 0)
        def _():
            chain_copy(1, PLANES - 1 - z, c).wait_recv()

        @pl.loop(0, part // STRIP)
        def _(s):
            at = pl.ds(multiple(z * token_count + c * part + s * STRIP, STRIP), STRIP)
            value = results[at, :].astype(jnp.float32) * scales[at, 0:1]
            above = sums[0, at, :].astype(jnp.float32)
            below = sums[1, at, :].astype(jnp.float32)
            value = value + jnp.where(z < PLANES - 1, above, 0.0)
            value = value + jnp.where(z > 0, below, 0.0)
            final[pl.ds(multiple(c * part + s * STRIP, STRIP), STRIP), :] = value.astype(
                jnp.bfloat16
            )

    store = pltpu.make_async_copy(final, combined, store_sem.at[0])
    store.start()

    for k in range(chunks):
        grad_copy(k).wait_send()
        y_copy(k).wait_send()
        for j in range(2):
            x_copy(j, k).wait_send()
        for j in range(4):
            core_copy(j, k).wait_send()
    for c in range(TOKEN_SPLITS):
        for hop in range(PLANES - 1):
            for direction in range(2):

                @pl.when(token_sends(direction, hop))
                def _():
                    token_copy(direction, hop, c).wait_send()

    for copy in table_copies:
        copy.wait_send()
    for second in range(2):
        chain_steps(second, drain_sums)
    store.wait()
    for k in range(chunks):
        for copy in moment_copies(k):
            copy.wait_send()
            copy.wait_recv()


def store_kernel(*refs):
    count = (len(refs) - 2) // 2
    results, outs = refs[:count], refs[count : 2 * count]
    staged, sem = refs[2 * count :]
    load = pltpu.make_async_copy(results[-1], staged, sem.at[count])
    load.start()
    copies = [
        pltpu.make_async_copy(results[i], outs[i], sem.at[i]) for i in range(count - 1)
    ]
    for copy in copies:
        copy.start()
    load.wait()
    copies.append(pltpu.make_async_copy(staged, outs[-1], sem.at[count - 1]))
    copies[-1].start()
    for copy in copies:
        copy.wait()


def store_call(results):
    any_space = pl.BlockSpec(memory_space=pl.ANY)
    return pl.pallas_call(
        store_kernel,
        name="store",
        out_shape=tuple(jax.ShapeDtypeStruct(out.shape, out.dtype) for out in results),
        in_specs=[any_space] * len(results),
        out_specs=(any_space,) * len(results),
        scratch_shapes=[
            pltpu.VMEM(results[-1].shape, results[-1].dtype),
            pltpu.SemaphoreType.DMA((len(results) + 1,)),
        ],
    )(*results)


def layer_call(
    mask,
    tokens,
    routes,
    combine_weight,
    w_in,
    w_out,
    grad_in,
    grad_out,
    first_in,
    second_in,
    first_out,
    second_out,
):
    token_count, width = tokens.shape
    half = width // 2
    hid = w_out.shape[0]
    lanes = 128
    any_space = pl.BlockSpec(memory_space=pl.ANY)
    bf16, dma = jnp.bfloat16, pltpu.SemaphoreType.DMA
    chunks = 3 * SPLITS
    outs = (tokens, first_in, second_in, first_out, second_out)
    rows = PLANES * token_count
    return pl.pallas_call(
        functools.partial(layer_kernel, mask),
        name=f"layer_{mask}",
        out_shape=tuple(jax.ShapeDtypeStruct(out.shape, out.dtype) for out in outs),
        in_specs=[any_space] * 11,
        out_specs=(any_space,) * 5,
        scratch_shapes=[
            pltpu.VMEM((rows, width), bf16),
            pltpu.VMEM(routes.shape[::-1], jnp.int32),
            pltpu.VMEM(routes.shape[::-1], jnp.float32),
            pltpu.VMEM((PLANES, 8, token_count), jnp.float32),
            pltpu.VMEM((3 * hid, half), bf16),
            pltpu.VMEM((3 * hid, half), bf16),
            pltpu.VMEM((3 * hid, half), bf16),
            pltpu.VMEM((3 * hid, half), bf16),
            pltpu.VMEM((3 * hid, half), bf16),
            pltpu.VMEM((3 * hid, half), bf16),
            pltpu.VMEM((3 * hid, half), bf16),
            pltpu.VMEM((3, 2, GROUP * hid, half), bf16),
            pltpu.VMEM((rows, GROUP * hid), bf16),
            pltpu.VMEM((rows, width), bf16),
            pltpu.VMEM((2, rows, width), bf16),
            pltpu.VMEM((rows, lanes), jnp.float32),
            pltpu.VMEM((token_count, width), bf16),
            dma((15,)),
            dma((2, chunks)),
            dma((2, chunks)),
            dma((2, 2, chunks)),
            dma((2, 4, chunks)),
            dma((2, 2, chunks)),
            dma((2, 2, PLANES - 1, TOKEN_SPLITS)),
            dma((2, PLANES - 1)),
            dma((2, 2, PLANES - 1, TOKEN_SPLITS)),
            dma((1,)),
        ],
        compiler_params=pltpu.CompilerParams(
            collective_id=mask, has_side_effects=True, vmem_limit_bytes=59 * 1024 * 1024
        ),
    )(
        tokens,
        routes.T,
        combine_weight.T,
        w_in,
        w_out,
        grad_in,
        grad_out,
        first_in,
        second_in,
        first_out,
        second_out,
    )


def exchanged(block, axis, mask):
    return lax.ppermute(block, axis, [(i, i ^ mask) for i in range(lax.axis_size(axis))])


def slot_ranks(flat_routes, expert_count):
    onehot = (flat_routes[:, None] == jnp.arange(expert_count, dtype=jnp.int32)[None, :]).astype(
        jnp.int32
    )
    ranks = jnp.cumsum(onehot, axis=0) - 1
    return jnp.sum(ranks * onehot, axis=1)


def times_rows(row_data, weight_rows):
    return lax.dot_general(
        row_data, weight_rows, (((1,), (1,)), ((), ())), preferred_element_type=jnp.float32
    )


def migrate_any(moment, source_rows, device_count):
    spread = lax.all_to_all(
        moment.reshape(device_count, -1), "expert", split_axis=0, concat_axis=0, tiled=True
    )
    picked = jnp.take(spread, source_rows, axis=0)
    landed = lax.all_to_all(picked, "expert", split_axis=0, concat_axis=0, tiled=True)
    return landed.reshape(moment.shape)


def summed_half(gradient, dp_index):
    half = gradient.shape[1] // 2
    kept = lax.dynamic_slice_in_dim(gradient, dp_index * half, half, 1)
    leaving = lax.dynamic_slice_in_dim(gradient, (1 - dp_index) * half, half, 1)
    return kept.astype(jnp.float32) + exchanged(leaving, "dp", 1).astype(jnp.float32)


def gathered(piece):
    pieces = {(0, 0): piece, (0, 1): exchanged(piece, "dp", 1)}
    for side in range(2):
        pieces[2, side] = exchanged(pieces[0, side], "expert", 2)
    for side in range(2):
        pieces[1, side] = exchanged(pieces[0, side], "expert", 1)
        pieces[3, side] = exchanged(pieces[2, side], "expert", 1)
    return pieces


def body(
    move,
    tokens,
    routes,
    combine_weight,
    w_in,
    w_out,
    grad_in,
    grad_out,
    first_in,
    second_in,
    first_out,
    second_out,
):
    device_count = lax.axis_size("expert")
    expert_count = device_count // GROUP
    token_count, route_count = routes.shape
    width = tokens.shape[1]
    half = width // 2
    capacity = GROUP * (
        (token_count * route_count * 4 + 3 * expert_count * GROUP - 1) // (3 * expert_count * GROUP)
    )
    dp_index = lax.axis_index("dp")
    my_group = lax.axis_index("expert") // GROUP

    flat_routes = routes.reshape(-1)
    ranks = slot_ranks(flat_routes, expert_count)
    relative = flat_routes ^ my_group
    targets = (relative * capacity + ranks).reshape(token_count, route_count)
    slot_ids = jnp.arange(expert_count * capacity, dtype=jnp.int32)
    selector = jnp.any(targets[None, :, :] == slot_ids[:, None, None], axis=2).astype(jnp.bfloat16)
    outgoing = jnp.dot(selector, tokens, preferred_element_type=jnp.float32).astype(jnp.bfloat16)
    outgoing = outgoing.reshape(expert_count, capacity, width)
    arrived = [outgoing[0]] + [
        exchanged(outgoing[mask], "expert", mask * GROUP) for mask in range(1, expert_count)
    ]

    weights = (w_in[0], w_in[1], w_out)
    gradients = (grad_in[0, 0], grad_in[0, 1], grad_out[0])
    firsts = (first_in[0], first_in[1], first_out)
    seconds = (second_in[0], second_in[1], second_out)
    sums = [summed_half(gradient, dp_index) for gradient in gradients]
    stepped = [adam_update(*arrays) for arrays in zip(weights, sums, firsts, seconds)]
    gate_pieces, up_pieces, out_pieces = [gathered(step[0]) for step in stepped]
    moved_first = [move(step[1]) for step in stepped]
    moved_second = [move(step[2]) for step in stepped]

    rows = jnp.concatenate(arrived, 0)
    sides = [
        lax.dynamic_slice_in_dim(rows, dp_index * half, half, 1),
        lax.dynamic_slice_in_dim(rows, (1 - dp_index) * half, half, 1),
    ]
    totals = [jnp.zeros((rows.shape[0], half), jnp.float32) for _ in range(2)]
    for quarter in (0, 1, 2, 3):
        gate = times_rows(sides[0], gate_pieces[quarter, 0]) + times_rows(
            sides[1], gate_pieces[quarter, 1]
        )
        upward = times_rows(sides[0], up_pieces[quarter, 0]) + times_rows(
            sides[1], up_pieces[quarter, 1]
        )
        hidden = (jax.nn.silu(gate) * upward).astype(jnp.bfloat16)
        for side in range(2):
            part = jnp.dot(
                hidden, out_pieces[quarter, side], preferred_element_type=jnp.float32
            ).astype(jnp.bfloat16)
            totals[side] = totals[side] + part.astype(jnp.float32)
    near, far = [total.astype(jnp.bfloat16) for total in totals]
    results = jnp.where(
        dp_index == 0, jnp.concatenate([near, far], 1), jnp.concatenate([far, near], 1)
    ).reshape(expert_count, capacity, width)
    returned = [results[0]] + [
        exchanged(results[mask], "expert", mask * GROUP) for mask in range(1, expert_count)
    ]
    by_slot = jnp.concatenate(returned, 0)
    weight_table = jnp.sum(
        jnp.where(targets[:, :, None] == slot_ids[None, None, :], combine_weight[:, :, None], 0.0),
        axis=1,
    )
    weight_high = weight_table.astype(jnp.bfloat16)
    weight_low = (weight_table - weight_high.astype(jnp.float32)).astype(jnp.bfloat16)
    combined = (
        jnp.dot(weight_high, by_slot, preferred_element_type=jnp.float32)
        + jnp.dot(weight_low, by_slot, preferred_element_type=jnp.float32)
    ).astype(jnp.bfloat16)
    return (
        combined,
        jnp.stack(moved_first[:2]),
        jnp.stack(moved_second[:2]),
        moved_first[2],
        moved_second[2],
    )


def local(tokens, routes, combine_weight, owner_plan, *state):
    device_count = lax.axis_size("expert")
    expert_count = device_count // GROUP
    operands = (tokens, routes, combine_weight) + state
    if expert_count == PLANES and lax.axis_size("dp") == 2:
        branches = [functools.partial(layer_call, mask) for mask in range(1, expert_count)]
        return store_call(lax.switch(owner_plan[0] - 1, branches, *operands))
    device_ids = jnp.arange(device_count, dtype=jnp.int32)
    source_rows = jnp.take(owner_plan, device_ids // GROUP) * GROUP + device_ids % GROUP
    return body(lambda moment: migrate_any(moment, source_rows, device_count), *operands)


def solution(mesh):
    in_specs = (
        P(("expert", "dp"), None),
        P(("expert", "dp"), None),
        P(("expert", "dp"), None),
        P(),
        P(None, "expert", "dp"),
        P("expert", "dp"),
        P("dp", None, "expert", None),
        P("dp", "expert", None),
        P(None, "expert", "dp"),
        P(None, "expert", "dp"),
        P("expert", "dp"),
        P("expert", "dp"),
    )
    out_specs = (
        P(("expert", "dp"), None),
        P(None, "expert", "dp"),
        P(None, "expert", "dp"),
        P("expert", "dp"),
        P("expert", "dp"),
    )
    return jax.shard_map(local, mesh=mesh, in_specs=in_specs, out_specs=out_specs, check_vma=False)
```

```python
import functools

import jax
import jax.numpy as jnp
from jax import lax
from jax.experimental import pallas as pl
from jax.experimental.pallas import tpu as pltpu
from jax.sharding import PartitionSpec as P

GROUP = 4

BETA_ONE = 0.9
BETA_TWO = 0.95
LEARNING_RATE = 0.005
EPSILON = 1e-08
CORRECT_FIRST = 1.0 / (1.0 - 0.9**10)
CORRECT_SECOND = 1.0 / (1.0 - 0.95**10)

PLANES = 4
SPLITS = 2
TOKEN_SPLITS = 2
ROW_TILE = 16
STRIP = 16
TILE = 256
MESH = pl.DeviceIdType.MESH


def adam_update(weight, gradient, first_moment, second_moment):
    first_next = BETA_ONE * first_moment.astype(jnp.float32) + (1.0 - BETA_ONE) * gradient
    second_next = (
        BETA_TWO * second_moment.astype(jnp.float32) + (1.0 - BETA_TWO) * gradient * gradient
    )
    stepped = weight.astype(jnp.float32) - LEARNING_RATE * (first_next * CORRECT_FIRST) / (
        jnp.sqrt(second_next * CORRECT_SECOND) + EPSILON
    )
    return (
        stepped.astype(jnp.bfloat16),
        first_next.astype(jnp.bfloat16),
        second_next.astype(jnp.bfloat16),
    )


def layer_kernel(
    mask,
    tokens,
    routes,
    combine_weight,
    w_in,
    w_out,
    grad_in,
    grad_out,
    first_in,
    second_in,
    first_out,
    second_out,
    combined,
    first_in_next,
    second_in_next,
    first_out_next,
    second_out_next,
    rows_all,
    own_routes,
    own_weights,
    table_all,
    kept,
    came,
    old_weight,
    old_first,
    old_second,
    new_first,
    new_second,
    gathered,
    hidden,
    results,
    sums,
    slots,
    spread,
    scales,
    final,
    load_sem,
    grad_sem,
    y_sem,
    x_sem,
    core_sem,
    moment_sem,
    token_sem,
    table_sem,
    chain_sem,
    store_sem,
):
    token_count, width = tokens.shape
    half = width // 2
    hid = w_out.shape[0]
    quarters = gathered.shape[2] // hid
    chunk = hid // SPLITS
    chunks = 3 * SPLITS
    part = width // TOKEN_SPLITS
    room = slots.shape[1]

    e = lax.axis_index("expert")
    y = lax.axis_index("dp")
    z = lax.div(e, quarters)
    mine = lax.rem(e, quarters)
    core = lax.rem(e, 2)
    side = lax.div(mine, 2)
    core_e = e + 1 - 2 * core
    x_e = e + 2 - 4 * side
    low = lax.rem(z, 2)
    high = lax.div(z, 2)

    def flipped(bits):
        moved = e
        if bits & 1:
            moved = moved + quarters * (1 - 2 * low)
        if bits & 2:
            moved = moved + 2 * quarters * (1 - 2 * high)
        return moved

    def multiple(value, factor):
        return pl.multiple_of(value, factor)

    def remote(src, dst, sem, index, target):
        return pltpu.make_async_remote_copy(
            src_ref=src,
            dst_ref=dst,
            send_sem=sem.at[(0,) + index],
            recv_sem=sem.at[(1,) + index],
            device_id=target,
            device_id_type=MESH,
        )

    def shard(pair, single, m):
        return pair.at[m] if m < 2 else single

    def gradient(m):
        return grad_in.at[0, m] if m < 2 else grad_out.at[0]

    stays = pl.ds(multiple(y * half, 128), half)
    leaves = pl.ds(multiple((1 - y) * half, 128), half)
    loads = []
    for m in range(3):
        block = pl.ds(m * hid, hid)
        loads.append(
            [
                pltpu.make_async_copy(src, dst.at[block], load_sem.at[4 * m + i])
                for i, (src, dst) in enumerate(
                    (
                        (gradient(m).at[:, stays], kept),
                        (shard(first_in, first_out, m), old_first),
                        (shard(second_in, second_out, m), old_second),
                        (shard(w_in, w_out, m), old_weight),
                    )
                )
            ]
        )
    own_rows = pl.ds(multiple(z * token_count, token_count), token_count)
    small = [
        pltpu.make_async_copy(routes, own_routes, load_sem.at[12]),
        pltpu.make_async_copy(combine_weight, own_weights, load_sem.at[13]),
        pltpu.make_async_copy(tokens, rows_all.at[own_rows], load_sem.at[14]),
    ]
    for load in small:
        load.start()
    for m in range(3):
        for load in loads[m]:
            load.start()

    barrier = pltpu.get_barrier_semaphore()
    for target in (
        (core_e, y),
        (x_e, y),
        (e, 1 - y),
        (flipped(1), y),
        (flipped(2), y),
        (flipped(3), y),
    ):
        pl.semaphore_signal(barrier, inc=1, device_id=target, device_id_type=MESH)

    for load in small[:2]:
        load.wait()
    experts = lax.broadcasted_iota(jnp.int32, table_all.shape[1:], 0)
    table = jnp.zeros(table_all.shape[1:], jnp.float32)
    for route in range(own_routes.shape[0]):
        named = experts == own_routes[route : route + 1, :]
        table = table + jnp.where(named, own_weights[route : route + 1, :], 0.0)
    table_all[z] = table

    pl.semaphore_wait(barrier, 6)

    def grad_copy(k):
        m, r = divmod(k, SPLITS)
        return remote(
            gradient(m).at[pl.ds(r * chunk, chunk), leaves],
            came.at[pl.ds(k * chunk, chunk)],
            grad_sem,
            (k,),
            (e, 1 - y),
        )

    inner = lax.rem(z + high, 2) == 1
    outer = jnp.logical_not(inner)
    end, near = (PLANES - 1) * high, 1 + high
    far, far_end = PLANES - 2 - high, (PLANES - 1) * (1 - high)

    def device_of(plane):
        return (e + (plane - z) * quarters, y)

    def plane_rows(plane, count):
        return pl.ds(multiple(plane * token_count, token_count), count)

    def columns(c):
        return pl.ds(c * part, part)

    picked = (near, far, far_end)

    def token_copy(message, c):
        plane = (end, near, end, *picked)[message]
        target = (near, far, far, end, end, end)[message]
        there = rows_all.at[plane_rows(plane, token_count if message < 3 else room), columns(c)]
        if message < 2:
            src = tokens.at[:, columns(c)]
        elif message == 2:
            src = there
        else:
            src = slots.at[message - 3, :, columns(c)]
        return remote(src, there, token_sem, (message, c), device_of(target))

    def slot_line(plane):
        line = table_all[plane, pl.ds(end, 1), :]
        named = line != 0.0
        before = lax.broadcasted_iota(jnp.int32, (token_count, token_count), 0) < (
            lax.broadcasted_iota(jnp.int32, (token_count, token_count), 1)
        )
        ranks = jnp.dot(
            jnp.broadcast_to(jnp.where(named, 1.0, 0.0), (8, token_count)).astype(jnp.bfloat16),
            jnp.where(before, 1.0, 0.0).astype(jnp.bfloat16),
            preferred_element_type=jnp.float32,
        )
        return jnp.where(named, ranks[0:1, :], -1.0)

    def pick_rows(which, c):
        plane = picked[which]
        slot = lax.broadcasted_iota(jnp.int32, (room, token_count), 0).astype(jnp.float32)
        chosen = jnp.where(slot == slot_line(plane), 1.0, 0.0).astype(jnp.bfloat16)

        @pl.loop(0, part // TILE)
        def _(t):
            at = pl.ds(multiple(c * part + t * TILE, TILE), TILE)
            slots[which, :, at] = jnp.dot(
                chosen,
                rows_all[plane_rows(plane, token_count), at],
                preferred_element_type=jnp.float32,
            ).astype(jnp.bfloat16)

        token_copy(3 + which, c).start()

    def relay_end_tokens(c):
        @pl.when(inner)
        def _():
            token_copy(0, c).wait_recv()
            token_copy(2, c).start()

    def pick_far_tokens(which, c):
        @pl.when(inner)
        def _():
            token_copy(which, c).wait_recv()
            pick_rows(which, c)

    table_copies = [
        remote(table_all.at[z], table_all.at[z], table_sem, (bits - 1,), (flipped(bits), y))
        for bits in range(1, PLANES)
    ]

    for k in range(chunks):
        grad_copy(k).start()
    for copy in table_copies:
        copy.start()
    for c in range(TOKEN_SPLITS):

        @pl.when(outer)
        def _():
            token_copy(0, c).start()

        @pl.when(inner)
        def _():
            token_copy(1, c).start()

    small[2].wait()
    for c in range(TOKEN_SPLITS):
        pl.when(inner)(functools.partial(pick_rows, 0, c))

    def weight_block(k, width_half, quarter):
        m, r = divmod(k, SPLITS)
        return gathered.at[
            m, width_half, pl.ds(multiple(quarter * hid + r * chunk, chunk), chunk)
        ]

    x_quarter = mine + 2 - 4 * side
    sources = ((y, mine), (1 - y, mine), (y, x_quarter), (1 - y, x_quarter))

    def y_copy(k):
        block = weight_block(k, y, mine)
        return remote(block, block, y_sem, (k,), (e, 1 - y))

    def x_copy(j, k):
        block = weight_block(k, *sources[j])
        return remote(block, block, x_sem, (j, k), (x_e, y))

    def core_copy(j, k):
        block = weight_block(k, *sources[j])
        return remote(block, block, core_sem, (j, k), (core_e, y))

    def moment_copies(k):
        m, r = divmod(k, SPLITS)
        here, there = pl.ds(k * chunk, chunk), pl.ds(r * chunk, chunk)
        return [
            remote(
                new.at[here],
                shard(pair, single, m).at[there],
                moment_sem,
                (i, k),
                (flipped(mask), y),
            )
            for i, (new, pair, single) in enumerate(
                (
                    (new_first, first_in_next, first_out_next),
                    (new_second, second_in_next, second_out_next),
                )
            )
        ]

    inner_first = chunks if mask == 1 else (2 * chunks) // 3
    outer_first = chunks if mask == 1 else chunks // 2

    def send_moments(which, start, stop):
        @pl.when(which)
        def _():
            for k in range(start, stop):
                for copy in moment_copies(k):
                    copy.start()

    for k in range(chunks):
        m, r = divmod(k, SPLITS)
        if r == 0:
            for load in loads[m]:
                load.wait()
        grad_copy(k).wait_recv()

        @pl.loop(0, chunk // STRIP)
        def _(i):
            at = pl.ds(multiple(k * chunk + i * STRIP, STRIP), STRIP)
            total = kept[at, :].astype(jnp.float32) + came[at, :].astype(jnp.float32)
            weight, first, second = adam_update(
                old_weight[at, :], total, old_first[at, :], old_second[at, :]
            )
            place = pl.ds(multiple(mine * hid + r * chunk + i * STRIP, STRIP), STRIP)
            gathered[m, y, place, :] = weight
            new_first[at, :] = first
            new_second[at, :] = second

        x_copy(0, k).start()
        y_copy(k).start()
        core_copy(0, k).start()
        if mask == 1:
            send_moments(outer, k, k + 1)
        if k == 1:
            for copy in table_copies:
                copy.wait_recv()
            relay_end_tokens(0)
        if k == 2:
            relay_end_tokens(1)
            pick_far_tokens(1, 0)
        if k == 3:
            pick_far_tokens(1, 1)
        if k == 4:
            pick_far_tokens(2, 0)
        if k == 5:
            pick_far_tokens(2, 1)
        if mask == 1 and k < 2:
            send_moments(inner, k, k + 1)
        if mask == 1 and k == 5:
            send_moments(inner, 2, inner_first)
        if mask != 1 and k == 2:
            send_moments(inner, 0, 3)
        if mask != 1 and k > 2:
            send_moments(inner, k, min(k + 1, inner_first))

    for k in range(chunks):
        y_copy(k).wait_recv()
        x_copy(1, k).start()
        core_copy(1, k).start()
        x_copy(0, k).wait_recv()
        core_copy(2, k).start()
        if mask != 1 and k == 0:
            send_moments(outer, 0, outer_first)
    for message in range(3, 6):
        for c in range(TOKEN_SPLITS):

            @pl.when(outer)
            def _():
                token_copy(message, c).wait_recv()

    diagonal = lax.broadcasted_iota(jnp.int32, (token_count, token_count), 0) == (
        lax.broadcasted_iota(jnp.int32, (token_count, token_count), 1)
    )

    def column(line):
        return jnp.sum(jnp.where(diagonal, line, 0.0), axis=1, keepdims=True)

    def keep_scale(which, plane, expert):
        scales[which, plane_rows(plane, token_count), :] = jnp.broadcast_to(
            column(table_all[plane, pl.ds(expert, 1), :]), (token_count, scales.shape[2])
        )

    for plane in range(PLANES):
        keep_scale(0, plane, z)

    @pl.when(inner)
    def _():
        lanes = lax.broadcasted_iota(jnp.int32, (token_count, token_count), 1)
        for which, plane in enumerate(picked):
            keep_scale(1, plane, end)
            spread[which] = jnp.where(
                lanes.astype(jnp.float32) == column(slot_line(plane)), 1.0, 0.0
            ).astype(jnp.bfloat16)
            rest = pl.ds(
                multiple(plane * token_count + room, ROW_TILE), token_count - room
            )
            sums[0, rest, :] = jnp.zeros((token_count - room, width), jnp.bfloat16)

    wide = 2 * SPLITS
    for k in range(wide):
        x_copy(1, k).wait_recv()
        core_copy(3, k).start()
    for k in range(wide):
        for j in range(4):
            core_copy(j, k).wait_recv()

    row_tiles = rows_all.shape[0] // TILE
    contract = (((1,), (1,)), ((), ()))

    @pl.loop(0, (quarters * hid // TILE) * row_tiles)
    def _(t):
        at = pl.ds(multiple(lax.rem(t, row_tiles) * TILE, TILE), TILE)
        units = pl.ds(multiple(lax.div(t, row_tiles) * TILE, TILE), TILE)

        def times_rows(m):
            return sum(
                lax.dot_general(
                    rows_all[at, s * half : (s + 1) * half],
                    gathered[m, s, units, :],
                    contract,
                    preferred_element_type=jnp.float32,
                )
                for s in range(2)
            )

        gate, upward = times_rows(0), times_rows(1)
        hidden[at, units] = (jax.nn.silu(gate) * upward).astype(jnp.bfloat16)

    def times_out(s):
        @pl.loop(0, (half // TILE) * row_tiles)
        def _(t):
            at = pl.ds(multiple(lax.rem(t, row_tiles) * TILE, TILE), TILE)
            from_column = lax.div(t, row_tiles) * TILE
            results[at, pl.ds(multiple(s * half + from_column, TILE), TILE)] = jnp.dot(
                hidden[at, :],
                gathered[2, s, :, pl.ds(multiple(from_column, TILE), TILE)],
                preferred_element_type=jnp.float32,
            ).astype(jnp.bfloat16)

    for k in range(wide, chunks):
        for j in (0, 2):
            core_copy(j, k).wait_recv()
    times_out(y)
    for k in range(wide, chunks):
        x_copy(1, k).wait_recv()
        core_copy(3, k).start()
    for k in range(wide, chunks):
        for j in (1, 3):
            core_copy(j, k).wait_recv()
    times_out(1 - y)

    def result_copy(message, c):
        plane = (far_end, far, near, far_end, far, end)[message]
        target = (near, near, near, far, far, end)[message]
        at = plane_rows(plane, room if message < 3 else token_count)
        return remote(
            results.at[at, columns(c)],
            sums.at[0 if message < 3 else 1, at, columns(c)],
            chain_sem,
            (message, c),
            device_of(target),
        )

    def tiles(c, body):
        @pl.loop(0, part // TILE)
        def _(t):
            body(pl.ds(multiple(c * part + t * TILE, TILE), TILE))

    def weighted(at, cols):
        return results[at, cols].astype(jnp.float32) * scales[0, at, 0:1]

    def from_end(which, at, cols):
        rows = jnp.dot(
            spread[which], sums[0, at, cols], preferred_element_type=jnp.float32
        )
        return rows * scales[1, at, 0:1]

    def far_sums(i, c):
        @pl.when(inner)
        def _():
            result_copy(i, c).wait_recv()
            at = plane_rows((far_end, far)[i], token_count)

            def body(cols):
                total = weighted(at, cols) + from_end(2 - i, at, cols)
                results[at, cols] = total.astype(jnp.bfloat16)

            tiles(c, body)
            result_copy(3 + i, c).start()

    def end_sums(c):
        @pl.when(inner)
        def _():
            result_copy(3, c).wait_recv()
            at = plane_rows(end, token_count)

            def body(cols):
                total = weighted(at, cols) + sums[1, at, cols].astype(jnp.float32)
                results[at, cols] = total.astype(jnp.bfloat16)

            tiles(c, body)
            result_copy(5, c).start()

    @pl.when(outer)
    def _():
        for message in range(3):
            for c in range(TOKEN_SPLITS):
                result_copy(message, c).start()

    if mask == 1:
        far_sums(0, 0)
        far_sums(0, 1)
        end_sums(0)
        far_sums(1, 0)
        end_sums(1)
        far_sums(1, 1)
    else:
        for i in range(2):
            for c in range(TOKEN_SPLITS):
                far_sums(i, c)
        send_moments(outer, outer_first, chunks)
        send_moments(inner, inner_first, chunks)
        for c in range(TOKEN_SPLITS):
            end_sums(c)

    for c in range(TOKEN_SPLITS):

        @pl.when(inner)
        def _():
            result_copy(2, c).wait_recv()
            result_copy(4, c).wait_recv()
            at = plane_rows(near, token_count)

            def body(cols):
                total = weighted(at, cols) + from_end(0, at, cols)
                total = total + sums[1, at, cols].astype(jnp.float32)
                final[:, cols] = total.astype(jnp.bfloat16)

            tiles(c, body)

        @pl.when(outer)
        def _():
            result_copy(5, c).wait_recv()
            at = plane_rows(end, token_count)

            def body(cols):
                total = weighted(at, cols) + sums[1, at, cols].astype(jnp.float32)
                final[:, cols] = total.astype(jnp.bfloat16)

            tiles(c, body)

    store = pltpu.make_async_copy(final, combined, store_sem.at[0])
    store.start()

    for k in range(chunks):
        grad_copy(k).wait_send()
        y_copy(k).wait_send()
        for j in range(2):
            x_copy(j, k).wait_send()
        for j in range(4):
            core_copy(j, k).wait_send()
    for c in range(TOKEN_SPLITS):

        @pl.when(outer)
        def _():
            token_copy(0, c).wait_send()
            for message in range(3):
                result_copy(message, c).wait_send()

        @pl.when(inner)
        def _():
            for message in range(1, 6):
                token_copy(message, c).wait_send()
            for message in range(3, 6):
                result_copy(message, c).wait_send()

    for copy in table_copies:
        copy.wait_send()
    store.wait()
    for k in range(chunks):
        for copy in moment_copies(k):
            copy.wait_send()
            copy.wait_recv()


def store_kernel(*refs):
    count = (len(refs) - 2) // 2
    results, outs = refs[:count], refs[count : 2 * count]
    staged, sem = refs[2 * count :]
    load = pltpu.make_async_copy(results[-1], staged, sem.at[count])
    load.start()
    copies = [
        pltpu.make_async_copy(results[i], outs[i], sem.at[i]) for i in range(count - 1)
    ]
    for copy in copies:
        copy.start()
    load.wait()
    copies.append(pltpu.make_async_copy(staged, outs[-1], sem.at[count - 1]))
    copies[-1].start()
    for copy in copies:
        copy.wait()


def store_call(results):
    any_space = pl.BlockSpec(memory_space=pl.ANY)
    return pl.pallas_call(
        store_kernel,
        name="store",
        out_shape=tuple(jax.ShapeDtypeStruct(out.shape, out.dtype) for out in results),
        in_specs=[any_space] * len(results),
        out_specs=(any_space,) * len(results),
        scratch_shapes=[
            pltpu.VMEM(results[-1].shape, results[-1].dtype),
            pltpu.SemaphoreType.DMA((len(results) + 1,)),
        ],
    )(*results)


def layer_call(
    mask,
    tokens,
    routes,
    combine_weight,
    w_in,
    w_out,
    grad_in,
    grad_out,
    first_in,
    second_in,
    first_out,
    second_out,
):
    token_count, width = tokens.shape
    half = width // 2
    hid = w_out.shape[0]
    lanes = 128
    any_space = pl.BlockSpec(memory_space=pl.ANY)
    bf16, dma = jnp.bfloat16, pltpu.SemaphoreType.DMA
    chunks = 3 * SPLITS
    outs = (tokens, first_in, second_in, first_out, second_out)
    rows = PLANES * token_count
    load = -(-token_count * routes.shape[1] * 4 // (3 * PLANES * GROUP)) * GROUP
    room = -(-load // ROW_TILE) * ROW_TILE
    return pl.pallas_call(
        functools.partial(layer_kernel, mask),
        name=f"layer_{mask}",
        out_shape=tuple(jax.ShapeDtypeStruct(out.shape, out.dtype) for out in outs),
        in_specs=[any_space] * 11,
        out_specs=(any_space,) * 5,
        scratch_shapes=[
            pltpu.VMEM((rows, width), bf16),
            pltpu.VMEM(routes.shape[::-1], jnp.int32),
            pltpu.VMEM(routes.shape[::-1], jnp.float32),
            pltpu.VMEM((PLANES, 8, token_count), jnp.float32),
            pltpu.VMEM((3 * hid, half), bf16),
            pltpu.VMEM((3 * hid, half), bf16),
            pltpu.VMEM((3 * hid, half), bf16),
            pltpu.VMEM((3 * hid, half), bf16),
            pltpu.VMEM((3 * hid, half), bf16),
            pltpu.VMEM((3 * hid, half), bf16),
            pltpu.VMEM((3 * hid, half), bf16),
            pltpu.VMEM((3, 2, GROUP * hid, half), bf16),
            pltpu.VMEM((rows, GROUP * hid), bf16),
            pltpu.VMEM((rows, width), bf16),
            pltpu.VMEM((2, rows, width), bf16),
            pltpu.VMEM((3, room, width), bf16),
            pltpu.VMEM((3, token_count, token_count), bf16),
            pltpu.VMEM((2, rows, lanes), jnp.float32),
            pltpu.VMEM((token_count, width), bf16),
            dma((15,)),
            dma((2, chunks)),
            dma((2, chunks)),
            dma((2, 2, chunks)),
            dma((2, 4, chunks)),
            dma((2, 2, chunks)),
            dma((2, 6, TOKEN_SPLITS)),
            dma((2, PLANES - 1)),
            dma((2, 6, TOKEN_SPLITS)),
            dma((1,)),
        ],
        compiler_params=pltpu.CompilerParams(
            collective_id=mask, has_side_effects=True, vmem_limit_bytes=59 * 1024 * 1024
        ),
    )(
        tokens,
        routes.T,
        combine_weight.T,
        w_in,
        w_out,
        grad_in,
        grad_out,
        first_in,
        second_in,
        first_out,
        second_out,
    )


def exchanged(block, axis, mask):
    return lax.ppermute(block, axis, [(i, i ^ mask) for i in range(lax.axis_size(axis))])


def slot_ranks(flat_routes, expert_count):
    onehot = (flat_routes[:, None] == jnp.arange(expert_count, dtype=jnp.int32)[None, :]).astype(
        jnp.int32
    )
    ranks = jnp.cumsum(onehot, axis=0) - 1
    return jnp.sum(ranks * onehot, axis=1)


def times_rows(row_data, weight_rows):
    return lax.dot_general(
        row_data, weight_rows, (((1,), (1,)), ((), ())), preferred_element_type=jnp.float32
    )


def migrate_any(moment, source_rows, device_count):
    spread = lax.all_to_all(
        moment.reshape(device_count, -1), "expert", split_axis=0, concat_axis=0, tiled=True
    )
    picked = jnp.take(spread, source_rows, axis=0)
    landed = lax.all_to_all(picked, "expert", split_axis=0, concat_axis=0, tiled=True)
    return landed.reshape(moment.shape)


def summed_half(gradient, dp_index):
    half = gradient.shape[1] // 2
    kept = lax.dynamic_slice_in_dim(gradient, dp_index * half, half, 1)
    leaving = lax.dynamic_slice_in_dim(gradient, (1 - dp_index) * half, half, 1)
    return kept.astype(jnp.float32) + exchanged(leaving, "dp", 1).astype(jnp.float32)


def gathered(piece):
    pieces = {(0, 0): piece, (0, 1): exchanged(piece, "dp", 1)}
    for side in range(2):
        pieces[2, side] = exchanged(pieces[0, side], "expert", 2)
    for side in range(2):
        pieces[1, side] = exchanged(pieces[0, side], "expert", 1)
        pieces[3, side] = exchanged(pieces[2, side], "expert", 1)
    return pieces


def body(
    move,
    tokens,
    routes,
    combine_weight,
    w_in,
    w_out,
    grad_in,
    grad_out,
    first_in,
    second_in,
    first_out,
    second_out,
):
    device_count = lax.axis_size("expert")
    expert_count = device_count // GROUP
    token_count, route_count = routes.shape
    width = tokens.shape[1]
    half = width // 2
    capacity = GROUP * (
        (token_count * route_count * 4 + 3 * expert_count * GROUP - 1) // (3 * expert_count * GROUP)
    )
    dp_index = lax.axis_index("dp")
    my_group = lax.axis_index("expert") // GROUP

    flat_routes = routes.reshape(-1)
    ranks = slot_ranks(flat_routes, expert_count)
    relative = flat_routes ^ my_group
    targets = (relative * capacity + ranks).reshape(token_count, route_count)
    slot_ids = jnp.arange(expert_count * capacity, dtype=jnp.int32)
    selector = jnp.any(targets[None, :, :] == slot_ids[:, None, None], axis=2).astype(jnp.bfloat16)
    outgoing = jnp.dot(selector, tokens, preferred_element_type=jnp.float32).astype(jnp.bfloat16)
    outgoing = outgoing.reshape(expert_count, capacity, width)
    arrived = [outgoing[0]] + [
        exchanged(outgoing[mask], "expert", mask * GROUP) for mask in range(1, expert_count)
    ]

    weights = (w_in[0], w_in[1], w_out)
    gradients = (grad_in[0, 0], grad_in[0, 1], grad_out[0])
    firsts = (first_in[0], first_in[1], first_out)
    seconds = (second_in[0], second_in[1], second_out)
    sums = [summed_half(gradient, dp_index) for gradient in gradients]
    stepped = [adam_update(*arrays) for arrays in zip(weights, sums, firsts, seconds)]
    gate_pieces, up_pieces, out_pieces = [gathered(step[0]) for step in stepped]
    moved_first = [move(step[1]) for step in stepped]
    moved_second = [move(step[2]) for step in stepped]

    rows = jnp.concatenate(arrived, 0)
    sides = [
        lax.dynamic_slice_in_dim(rows, dp_index * half, half, 1),
        lax.dynamic_slice_in_dim(rows, (1 - dp_index) * half, half, 1),
    ]
    totals = [jnp.zeros((rows.shape[0], half), jnp.float32) for _ in range(2)]
    for quarter in (0, 1, 2, 3):
        gate = times_rows(sides[0], gate_pieces[quarter, 0]) + times_rows(
            sides[1], gate_pieces[quarter, 1]
        )
        upward = times_rows(sides[0], up_pieces[quarter, 0]) + times_rows(
            sides[1], up_pieces[quarter, 1]
        )
        hidden = (jax.nn.silu(gate) * upward).astype(jnp.bfloat16)
        for side in range(2):
            part = jnp.dot(
                hidden, out_pieces[quarter, side], preferred_element_type=jnp.float32
            ).astype(jnp.bfloat16)
            totals[side] = totals[side] + part.astype(jnp.float32)
    near, far = [total.astype(jnp.bfloat16) for total in totals]
    results = jnp.where(
        dp_index == 0, jnp.concatenate([near, far], 1), jnp.concatenate([far, near], 1)
    ).reshape(expert_count, capacity, width)
    returned = [results[0]] + [
        exchanged(results[mask], "expert", mask * GROUP) for mask in range(1, expert_count)
    ]
    by_slot = jnp.concatenate(returned, 0)
    weight_table = jnp.sum(
        jnp.where(targets[:, :, None] == slot_ids[None, None, :], combine_weight[:, :, None], 0.0),
        axis=1,
    )
    weight_high = weight_table.astype(jnp.bfloat16)
    weight_low = (weight_table - weight_high.astype(jnp.float32)).astype(jnp.bfloat16)
    combined = (
        jnp.dot(weight_high, by_slot, preferred_element_type=jnp.float32)
        + jnp.dot(weight_low, by_slot, preferred_element_type=jnp.float32)
    ).astype(jnp.bfloat16)
    return (
        combined,
        jnp.stack(moved_first[:2]),
        jnp.stack(moved_second[:2]),
        moved_first[2],
        moved_second[2],
    )


def local(tokens, routes, combine_weight, owner_plan, *state):
    device_count = lax.axis_size("expert")
    expert_count = device_count // GROUP
    operands = (tokens, routes, combine_weight) + state
    if expert_count == PLANES and lax.axis_size("dp") == 2:
        branches = [functools.partial(layer_call, mask) for mask in range(1, expert_count)]
        return store_call(lax.switch(owner_plan[0] - 1, branches, *operands))
    device_ids = jnp.arange(device_count, dtype=jnp.int32)
    source_rows = jnp.take(owner_plan, device_ids // GROUP) * GROUP + device_ids % GROUP
    return body(lambda moment: migrate_any(moment, source_rows, device_count), *operands)


def solution(mesh):
    in_specs = (
        P(("expert", "dp"), None),
        P(("expert", "dp"), None),
        P(("expert", "dp"), None),
        P(),
        P(None, "expert", "dp"),
        P("expert", "dp"),
        P("dp", None, "expert", None),
        P("dp", "expert", None),
        P(None, "expert", "dp"),
        P(None, "expert", "dp"),
        P("expert", "dp"),
        P("expert", "dp"),
    )
    out_specs = (
        P(("expert", "dp"), None),
        P(None, "expert", "dp"),
        P(None, "expert", "dp"),
        P("expert", "dp"),
        P("expert", "dp"),
    )
    return jax.shard_map(local, mesh=mesh, in_specs=in_specs, out_specs=out_specs, check_vma=False)
```

```python
import functools

import jax
import jax.numpy as jnp
from jax import lax
from jax.experimental import pallas as pl
from jax.experimental.pallas import tpu as pltpu
from jax.sharding import PartitionSpec as P

GROUP = 4

BETA_ONE = 0.9
BETA_TWO = 0.95
LEARNING_RATE = 0.005
EPSILON = 1e-08
CORRECT_FIRST = 1.0 / (1.0 - 0.9**10)
CORRECT_SECOND = 1.0 / (1.0 - 0.95**10)

PLANES = 4
SPLITS = 2
TOKEN_SPLITS = 2
ROW_TILE = 16
SEND_COUNTS = {"grad": 1, "y": 1, "x": 2, "core": 4, "moment": 2, "token": 6, "table": 1, "result": 6}
SENDS = {
    kind: sum(list(SEND_COUNTS.values())[:place]) for place, kind in enumerate(SEND_COUNTS)
}
STRIP = 16
TILE = 256
MESH = pl.DeviceIdType.MESH


def adam_update(weight, gradient, first_moment, second_moment):
    first_next = BETA_ONE * first_moment.astype(jnp.float32) + (1.0 - BETA_ONE) * gradient
    second_next = (
        BETA_TWO * second_moment.astype(jnp.float32) + (1.0 - BETA_TWO) * gradient * gradient
    )
    stepped = weight.astype(jnp.float32) - LEARNING_RATE * (first_next * CORRECT_FIRST) / (
        jnp.sqrt(second_next * CORRECT_SECOND) + EPSILON
    )
    return (
        stepped.astype(jnp.bfloat16),
        first_next.astype(jnp.bfloat16),
        second_next.astype(jnp.bfloat16),
    )


def layer_kernel(
    mask,
    tokens,
    routes,
    combine_weight,
    w_in,
    w_out,
    grad_in,
    grad_out,
    first_in,
    second_in,
    first_out,
    second_out,
    combined,
    first_in_next,
    second_in_next,
    first_out_next,
    second_out_next,
    rows_all,
    own_routes,
    own_weights,
    table_all,
    kept,
    came,
    old_weight,
    old_first,
    old_second,
    new_first,
    new_second,
    gathered,
    hidden,
    results,
    sums,
    slots,
    spread,
    scales,
    final,
    load_sem,
    send_sem,
    grad_sem,
    y_sem,
    x_sem,
    core_sem,
    moment_sem,
    token_sem,
    table_sem,
    result_sem,
):
    token_count, width = tokens.shape
    half = width // 2
    hid = w_out.shape[0]
    quarters = gathered.shape[2] // hid
    chunk = hid // SPLITS
    chunks = 3 * SPLITS
    part = width // TOKEN_SPLITS
    room = slots.shape[1]

    e = lax.axis_index("expert")
    y = lax.axis_index("dp")
    z = lax.div(e, quarters)
    mine = lax.rem(e, quarters)
    core = lax.rem(e, 2)
    side = lax.div(mine, 2)
    core_e = e + 1 - 2 * core
    x_e = e + 2 - 4 * side
    low = lax.rem(z, 2)
    high = lax.div(z, 2)

    def flipped(bits):
        moved = e
        if bits & 1:
            moved = moved + quarters * (1 - 2 * low)
        if bits & 2:
            moved = moved + 2 * quarters * (1 - 2 * high)
        return moved

    def multiple(value, factor):
        return pl.multiple_of(value, factor)

    def remote(src, dst, kind, sent, arrived, target):
        return pltpu.make_async_remote_copy(
            src_ref=src,
            dst_ref=dst,
            send_sem=send_sem.at[SENDS[kind] + sent],
            recv_sem=arrived,
            device_id=target,
            device_id_type=MESH,
        )

    def wait_sent(kind, sent, ref):
        remote(ref, ref, kind, sent, table_sem.at[0], (e, 1 - y)).wait_send()

    def wait_arrived(arrived, ref):
        remote(ref, ref, "grad", 0, arrived, (e, 1 - y)).wait_recv()

    def shard(pair, single, m):
        return pair.at[m] if m < 2 else single

    def gradient(m):
        return grad_in.at[0, m] if m < 2 else grad_out.at[0]

    stays = pl.ds(multiple(y * half, 128), half)
    leaves = pl.ds(multiple((1 - y) * half, 128), half)
    loads = []
    for m in range(3):
        block = pl.ds(m * hid, hid)
        loads.append(
            [
                pltpu.make_async_copy(src, dst.at[block], load_sem.at[m])
                for src, dst in (
                    (gradient(m).at[:, stays], kept),
                    (shard(first_in, first_out, m), old_first),
                    (shard(second_in, second_out, m), old_second),
                    (shard(w_in, w_out, m), old_weight),
                )
            ]
        )
    own_rows = pl.ds(multiple(z * token_count, token_count), token_count)
    small = [
        pltpu.make_async_copy(routes, own_routes, load_sem.at[3]),
        pltpu.make_async_copy(combine_weight, own_weights, load_sem.at[4]),
        pltpu.make_async_copy(tokens, rows_all.at[own_rows], load_sem.at[5]),
    ]
    for load in small:
        load.start()
    for m in range(3):
        for load in loads[m]:
            load.start()

    barrier = pltpu.get_barrier_semaphore()
    for target in (
        (core_e, y),
        (x_e, y),
        (e, 1 - y),
        (flipped(1), y),
        (flipped(2), y),
        (flipped(3), y),
    ):
        pl.semaphore_signal(barrier, inc=1, device_id=target, device_id_type=MESH)

    for load in small[:2]:
        load.wait()
    experts = lax.broadcasted_iota(jnp.int32, table_all.shape[1:], 0)
    table = jnp.zeros(table_all.shape[1:], jnp.float32)
    for route in range(own_routes.shape[0]):
        named = experts == own_routes[route : route + 1, :]
        table = table + jnp.where(named, own_weights[route : route + 1, :], 0.0)
    table_all[z] = table

    pl.semaphore_wait(barrier, 6)

    def grad_copy(k):
        m, r = divmod(k, SPLITS)
        return remote(
            gradient(m).at[pl.ds(r * chunk, chunk), leaves],
            came.at[pl.ds(k * chunk, chunk)],
            "grad",
            0,
            grad_sem.at[k],
            (e, 1 - y),
        )

    inner = lax.rem(z + high, 2) == 1
    outer = jnp.logical_not(inner)
    end, near = (PLANES - 1) * high, 1 + high
    far, far_end = PLANES - 2 - high, (PLANES - 1) * (1 - high)

    def device_of(plane):
        return (e + (plane - z) * quarters, y)

    def plane_rows(plane, count):
        return pl.ds(multiple(plane * token_count, token_count), count)

    def columns(c):
        return pl.ds(c * part, part)

    picked = (near, far, far_end)

    def token_copy(message, c):
        plane = (end, near, end, *picked)[message]
        target = (near, far, far, end, end, end)[message]
        there = rows_all.at[plane_rows(plane, token_count if message < 3 else room), columns(c)]
        if message < 3:
            src = there
        else:
            src = slots.at[message - 3, :, columns(c)]
        return remote(
            src, there, "token", message, token_sem.at[message, c], device_of(target)
        )

    def slot_line(plane):
        line = table_all[plane, pl.ds(end, 1), :]
        named = line != 0.0
        before = lax.broadcasted_iota(jnp.int32, (token_count, token_count), 0) < (
            lax.broadcasted_iota(jnp.int32, (token_count, token_count), 1)
        )
        ranks = jnp.dot(
            jnp.broadcast_to(jnp.where(named, 1.0, 0.0), (8, token_count)).astype(jnp.bfloat16),
            jnp.where(before, 1.0, 0.0).astype(jnp.bfloat16),
            preferred_element_type=jnp.float32,
        )
        return jnp.where(named, ranks[0:1, :], -1.0)

    def pick_rows(which, c):
        plane = picked[which]
        slot = lax.broadcasted_iota(jnp.int32, (room, token_count), 0).astype(jnp.float32)
        chosen = jnp.where(slot == slot_line(plane), 1.0, 0.0).astype(jnp.bfloat16)

        @pl.loop(0, part // TILE)
        def _(t):
            at = pl.ds(multiple(c * part + t * TILE, TILE), TILE)
            slots[which, :, at] = jnp.dot(
                chosen,
                rows_all[plane_rows(plane, token_count), at],
                preferred_element_type=jnp.float32,
            ).astype(jnp.bfloat16)

        token_copy(3 + which, c).start()

    def relay_end_tokens(c):
        @pl.when(inner)
        def _():
            token_copy(0, c).wait_recv()
            token_copy(2, c).start()

    def pick_far_tokens(which, c):
        @pl.when(inner)
        def _():
            token_copy(which, c).wait_recv()
            pick_rows(which, c)

    table_copies = [
        remote(
            table_all.at[z], table_all.at[z], "table", 0, table_sem.at[0], (flipped(bits), y)
        )
        for bits in range(1, PLANES)
    ]

    small[2].wait()
    for copy in table_copies:
        copy.start()
    for c in range(TOKEN_SPLITS):

        @pl.when(outer)
        def _():
            token_copy(0, c).start()

        @pl.when(inner)
        def _():
            token_copy(1, c).start()

    for k in range(chunks):
        grad_copy(k).start()
    for c in range(TOKEN_SPLITS):
        pl.when(inner)(functools.partial(pick_rows, 0, c))

    def weight_block(k, width_half, quarter):
        m, r = divmod(k, SPLITS)
        return gathered.at[
            m, width_half, pl.ds(multiple(quarter * hid + r * chunk, chunk), chunk)
        ]

    x_quarter = mine + 2 - 4 * side
    sources = ((y, mine), (1 - y, mine), (y, x_quarter), (1 - y, x_quarter))

    def y_copy(k):
        block = weight_block(k, y, mine)
        return remote(block, block, "y", 0, y_sem.at[k], (e, 1 - y))

    def x_copy(j, k):
        block = weight_block(k, *sources[j])
        return remote(block, block, "x", j, x_sem.at[j, k], (x_e, y))

    def core_copy(j, k):
        block = weight_block(k, *sources[j])
        return remote(
            block, block, "core", j, core_sem.at[j, k // (2 * SPLITS)], (core_e, y)
        )

    def moment_copies(k):
        m, r = divmod(k, SPLITS)
        here, there = pl.ds(k * chunk, chunk), pl.ds(r * chunk, chunk)
        return [
            remote(
                new.at[here],
                shard(pair, single, m).at[there],
                "moment",
                i,
                moment_sem.at[i],
                (flipped(mask), y),
            )
            for i, (new, pair, single) in enumerate(
                (
                    (new_first, first_in_next, first_out_next),
                    (new_second, second_in_next, second_out_next),
                )
            )
        ]

    pace = SPLITS // 2
    inner_first = chunks if mask == 1 else (2 * chunks) // 3
    outer_first = chunks if mask == 1 else chunks // 2

    def send_moments(which, start, stop):
        @pl.when(which)
        def _():
            for k in range(start, stop):
                for copy in moment_copies(k):
                    copy.start()

    for k in range(chunks):
        m, r = divmod(k, SPLITS)
        if r == 0:
            four = gathered.at[0, 0, pl.ds(0, len(loads[m]) * hid)]
            pltpu.make_async_copy(four, four, load_sem.at[m]).wait()
        grad_copy(k).wait_recv()

        @pl.loop(0, chunk // STRIP)
        def _(i):
            at = pl.ds(multiple(k * chunk + i * STRIP, STRIP), STRIP)
            total = kept[at, :].astype(jnp.float32) + came[at, :].astype(jnp.float32)
            weight, first, second = adam_update(
                old_weight[at, :], total, old_first[at, :], old_second[at, :]
            )
            place = pl.ds(multiple(mine * hid + r * chunk + i * STRIP, STRIP), STRIP)
            gathered[m, y, place, :] = weight
            new_first[at, :] = first
            new_second[at, :] = second

        x_copy(0, k).start()
        y_copy(k).start()
        core_copy(0, k).start()
        if mask == 1:
            send_moments(outer, k, k + 1)
        if (k + 1) % pace:
            continue
        stage = k // pace
        if stage == 1:
            wait_arrived(table_sem.at[0], table_all.at[pl.ds(0, PLANES - 1)])
            relay_end_tokens(0)
        if stage == 2:
            relay_end_tokens(1)
            pick_far_tokens(1, 0)
        if stage == 3:
            pick_far_tokens(1, 1)
        if stage == 4:
            pick_far_tokens(2, 0)
        if stage == 5:
            pick_far_tokens(2, 1)
        if mask == 1 and stage < 2:
            send_moments(inner, stage * pace, (stage + 1) * pace)
        if mask == 1 and stage == 5:
            send_moments(inner, 2 * pace, inner_first)
        if mask != 1 and stage == 2:
            send_moments(inner, 0, 3 * pace)
        if mask != 1 and stage == 3:
            send_moments(inner, 3 * pace, inner_first)

    for k in range(chunks):
        y_copy(k).wait_recv()
        x_copy(1, k).start()
        core_copy(1, k).start()
        x_copy(0, k).wait_recv()
        core_copy(2, k).start()
        if mask != 1 and k == pace - 1:
            send_moments(outer, 0, outer_first)
    for message in range(3, 6):
        for c in range(TOKEN_SPLITS):

            @pl.when(outer)
            def _():
                token_copy(message, c).wait_recv()

    diagonal = lax.broadcasted_iota(jnp.int32, (token_count, token_count), 0) == (
        lax.broadcasted_iota(jnp.int32, (token_count, token_count), 1)
    )

    def column(line):
        return jnp.sum(jnp.where(diagonal, line, 0.0), axis=1, keepdims=True)

    def keep_scale(which, plane, expert):
        scales[which, plane_rows(plane, token_count), :] = jnp.broadcast_to(
            column(table_all[plane, pl.ds(expert, 1), :]), (token_count, scales.shape[2])
        )

    for plane in range(PLANES):
        keep_scale(0, plane, z)

    @pl.when(inner)
    def _():
        lanes = lax.broadcasted_iota(jnp.int32, (token_count, token_count), 1)
        for which, plane in enumerate(picked):
            keep_scale(1, plane, end)
            spread[which] = jnp.where(
                lanes.astype(jnp.float32) == column(slot_line(plane)), 1.0, 0.0
            ).astype(jnp.bfloat16)
            rest = pl.ds(
                multiple(plane * token_count + room, ROW_TILE), token_count - room
            )
            sums[0, rest, :] = jnp.zeros((token_count - room, width), jnp.bfloat16)

    wide = 2 * SPLITS
    for k in range(wide):
        x_copy(1, k).wait_recv()
        core_copy(3, k).start()
    for j in range(4):
        wait_arrived(core_sem.at[j, 0], came.at[pl.ds(0, 2 * hid)])

    row_tiles = rows_all.shape[0] // TILE
    contract = (((1,), (1,)), ((), ()))

    @pl.loop(0, (quarters * hid // TILE) * row_tiles)
    def _(t):
        at = pl.ds(multiple(lax.rem(t, row_tiles) * TILE, TILE), TILE)
        units = pl.ds(multiple(lax.div(t, row_tiles) * TILE, TILE), TILE)

        def times_rows(m):
            return sum(
                lax.dot_general(
                    rows_all[at, s * half : (s + 1) * half],
                    gathered[m, s, units, :],
                    contract,
                    preferred_element_type=jnp.float32,
                )
                for s in range(2)
            )

        gate, upward = times_rows(0), times_rows(1)
        hidden[at, units] = (jax.nn.silu(gate) * upward).astype(jnp.bfloat16)

    def times_out(s):
        @pl.loop(0, (half // TILE) * row_tiles)
        def _(t):
            at = pl.ds(multiple(lax.rem(t, row_tiles) * TILE, TILE), TILE)
            from_column = lax.div(t, row_tiles) * TILE
            results[at, pl.ds(multiple(s * half + from_column, TILE), TILE)] = jnp.dot(
                hidden[at, :],
                gathered[2, s, :, pl.ds(multiple(from_column, TILE), TILE)],
                preferred_element_type=jnp.float32,
            ).astype(jnp.bfloat16)

    for j in (0, 2):
        wait_arrived(core_sem.at[j, 1], came.at[pl.ds(2 * hid, hid)])
    times_out(y)
    for k in range(wide, chunks):
        x_copy(1, k).wait_recv()
        core_copy(3, k).start()
    for j in (1, 3):
        wait_arrived(core_sem.at[j, 1], came.at[pl.ds(2 * hid, hid)])
    times_out(1 - y)

    def result_copy(message, c):
        plane = (far_end, far, near, far_end, far, end)[message]
        target = (near, near, near, far, far, end)[message]
        at = plane_rows(plane, room if message < 3 else token_count)
        return remote(
            results.at[at, columns(c)],
            sums.at[0 if message < 3 else 1, at, columns(c)],
            "result",
            message,
            result_sem.at[message, c],
            device_of(target),
        )

    def tiles(c, body):
        @pl.loop(0, part // TILE)
        def _(t):
            body(pl.ds(multiple(c * part + t * TILE, TILE), TILE))

    def weighted(at, cols):
        return results[at, cols].astype(jnp.float32) * scales[0, at, 0:1]

    def from_end(which, at, cols):
        rows = jnp.dot(
            spread[which], sums[0, at, cols], preferred_element_type=jnp.float32
        )
        return rows * scales[1, at, 0:1]

    def far_sums(i, c):
        @pl.when(inner)
        def _():
            result_copy(i, c).wait_recv()
            at = plane_rows((far_end, far)[i], token_count)

            def body(cols):
                total = weighted(at, cols) + from_end(2 - i, at, cols)
                results[at, cols] = total.astype(jnp.bfloat16)

            tiles(c, body)
            result_copy(3 + i, c).start()

    def end_sums(c):
        @pl.when(inner)
        def _():
            result_copy(3, c).wait_recv()
            at = plane_rows(end, token_count)

            def body(cols):
                total = weighted(at, cols) + sums[1, at, cols].astype(jnp.float32)
                results[at, cols] = total.astype(jnp.bfloat16)

            tiles(c, body)
            result_copy(5, c).start()

    @pl.when(outer)
    def _():
        for message in range(3):
            for c in range(TOKEN_SPLITS):
                result_copy(message, c).start()

    if mask == 1:
        far_sums(0, 0)
        far_sums(0, 1)
        end_sums(0)
        far_sums(1, 0)
        end_sums(1)
        far_sums(1, 1)
    else:
        for i in range(2):
            for c in range(TOKEN_SPLITS):
                if mask == 2 and i == 1 and c == 1:
                    send_moments(inner, inner_first, chunks)
                far_sums(i, c)
        send_moments(outer, outer_first, chunks)
        if mask == 3:
            send_moments(inner, inner_first, chunks)
        for c in range(TOKEN_SPLITS):
            end_sums(c)

    def drain_moments():
        for i in range(2):
            wait_sent("moment", i, came)
            wait_arrived(moment_sem.at[i], came)

    wait_sent("grad", 0, came)
    wait_sent("y", 0, came)
    for j in range(2):
        wait_sent("x", j, came)
    for j in range(4):
        wait_sent("core", j, came)
    wait_sent("table", 0, table_all.at[pl.ds(0, PLANES - 1)])
    all_rows, slot_rows = rows_all.at[pl.ds(0, token_count)], rows_all.at[pl.ds(0, room)]

    @pl.when(outer)
    def _():
        wait_sent("token", 0, all_rows)

    @pl.when(inner)
    def _():
        for message in range(1, 6):
            wait_sent("token", message, all_rows if message < 3 else slot_rows)

    if mask != 3:
        drain_moments()


    def add_far(message, plane, c):
        result_copy(message, c).wait_recv()
        at = plane_rows(plane, token_count)

        def body(cols):
            total = final[:, cols] + sums[1, at, cols].astype(jnp.float32)
            combined[:, cols] = total.astype(jnp.bfloat16)

        tiles(c, body)

    @pl.when(inner)
    def _():
        at = plane_rows(near, token_count)

        def body(cols):
            final[:, cols] = weighted(at, cols) + from_end(0, at, cols)

        for c in range(TOKEN_SPLITS):
            result_copy(2, c).wait_recv()
            tiles(c, body)
        for c in range(TOKEN_SPLITS):
            add_far(4, near, c)

    @pl.when(outer)
    def _():
        at = plane_rows(end, token_count)

        def body(cols):
            final[:, cols] = weighted(at, cols)

        for c in range(TOKEN_SPLITS):
            tiles(c, body)
        for c in range(TOKEN_SPLITS):
            add_far(5, end, c)

    @pl.when(outer)
    def _():
        for message in range(3):
            wait_sent("result", message, slot_rows)

    @pl.when(inner)
    def _():
        for message in range(3, 6):
            wait_sent("result", message, all_rows)

    if mask == 3:
        drain_moments()


def store_kernel(*refs):
    count = (len(refs) - 2) // 2
    results, outs = refs[:count], refs[count : 2 * count]
    staged, sem = refs[2 * count :]
    load = pltpu.make_async_copy(results[-1], staged, sem.at[count])
    load.start()
    copies = [
        pltpu.make_async_copy(results[i], outs[i], sem.at[i]) for i in range(count - 1)
    ]
    for copy in copies:
        copy.start()
    load.wait()
    copies.append(pltpu.make_async_copy(staged, outs[-1], sem.at[count - 1]))
    copies[-1].start()
    for copy in copies:
        copy.wait()


def store_call(results):
    any_space = pl.BlockSpec(memory_space=pl.ANY)
    return pl.pallas_call(
        store_kernel,
        name="store",
        out_shape=tuple(jax.ShapeDtypeStruct(out.shape, out.dtype) for out in results),
        in_specs=[any_space] * len(results),
        out_specs=(any_space,) * len(results),
        scratch_shapes=[
            pltpu.VMEM(results[-1].shape, results[-1].dtype),
            pltpu.SemaphoreType.DMA((len(results) + 1,)),
        ],
    )(*results)


def layer_call(
    mask,
    tokens,
    routes,
    combine_weight,
    w_in,
    w_out,
    grad_in,
    grad_out,
    first_in,
    second_in,
    first_out,
    second_out,
):
    token_count, width = tokens.shape
    half = width // 2
    hid = w_out.shape[0]
    lanes = 128
    any_space = pl.BlockSpec(memory_space=pl.ANY)
    bf16, dma = jnp.bfloat16, pltpu.SemaphoreType.DMA
    chunks = 3 * SPLITS
    outs = (tokens, first_in, second_in, first_out, second_out)
    rows = PLANES * token_count
    load = -(-token_count * routes.shape[1] * 4 // (3 * PLANES * GROUP)) * GROUP
    room = -(-load // ROW_TILE) * ROW_TILE
    return pl.pallas_call(
        functools.partial(layer_kernel, mask),
        name=f"layer_{mask}",
        out_shape=tuple(jax.ShapeDtypeStruct(out.shape, out.dtype) for out in outs),
        in_specs=[any_space] * 11,
        out_specs=(pl.BlockSpec(memory_space=pltpu.VMEM),) + (any_space,) * 4,
        scratch_shapes=[
            pltpu.VMEM((rows, width), bf16),
            pltpu.VMEM(routes.shape[::-1], jnp.int32),
            pltpu.VMEM(routes.shape[::-1], jnp.float32),
            pltpu.VMEM((PLANES, 8, token_count), jnp.float32),
            pltpu.VMEM((3 * hid, half), bf16),
            pltpu.VMEM((3 * hid, half), bf16),
            pltpu.VMEM((3 * hid, half), bf16),
            pltpu.VMEM((3 * hid, half), bf16),
            pltpu.VMEM((3 * hid, half), bf16),
            pltpu.VMEM((3 * hid, half), bf16),
            pltpu.VMEM((3 * hid, half), bf16),
            pltpu.VMEM((3, 2, GROUP * hid, half), bf16),
            pltpu.VMEM((rows, GROUP * hid), bf16),
            pltpu.VMEM((rows, width), bf16),
            pltpu.VMEM((2, rows, width), bf16),
            pltpu.VMEM((3, room, width), bf16),
            pltpu.VMEM((3, token_count, token_count), bf16),
            pltpu.VMEM((2, rows, lanes), jnp.float32),
            pltpu.VMEM((token_count, width), jnp.float32),
            dma((6,)),
            dma((sum(SEND_COUNTS.values()),)),
            dma((chunks,)),
            dma((chunks,)),
            dma((2, chunks)),
            dma((4, 2)),
            dma((2,)),
            dma((6, TOKEN_SPLITS)),
            dma((1,)),
            dma((6, TOKEN_SPLITS)),
        ],
        compiler_params=pltpu.CompilerParams(
            collective_id=mask, has_side_effects=True, vmem_limit_bytes=59 * 1024 * 1024
        ),
    )(
        tokens,
        routes.T,
        combine_weight.T,
        w_in,
        w_out,
        grad_in,
        grad_out,
        first_in,
        second_in,
        first_out,
        second_out,
    )


def exchanged(block, axis, mask):
    return lax.ppermute(block, axis, [(i, i ^ mask) for i in range(lax.axis_size(axis))])


def slot_ranks(flat_routes, expert_count):
    onehot = (flat_routes[:, None] == jnp.arange(expert_count, dtype=jnp.int32)[None, :]).astype(
        jnp.int32
    )
    ranks = jnp.cumsum(onehot, axis=0) - 1
    return jnp.sum(ranks * onehot, axis=1)


def times_rows(row_data, weight_rows):
    return lax.dot_general(
        row_data, weight_rows, (((1,), (1,)), ((), ())), preferred_element_type=jnp.float32
    )


def migrate_any(moment, source_rows, device_count):
    spread = lax.all_to_all(
        moment.reshape(device_count, -1), "expert", split_axis=0, concat_axis=0, tiled=True
    )
    picked = jnp.take(spread, source_rows, axis=0)
    landed = lax.all_to_all(picked, "expert", split_axis=0, concat_axis=0, tiled=True)
    return landed.reshape(moment.shape)


def summed_half(gradient, dp_index):
    half = gradient.shape[1] // 2
    kept = lax.dynamic_slice_in_dim(gradient, dp_index * half, half, 1)
    leaving = lax.dynamic_slice_in_dim(gradient, (1 - dp_index) * half, half, 1)
    return kept.astype(jnp.float32) + exchanged(leaving, "dp", 1).astype(jnp.float32)


def gathered(piece):
    pieces = {(0, 0): piece, (0, 1): exchanged(piece, "dp", 1)}
    for side in range(2):
        pieces[2, side] = exchanged(pieces[0, side], "expert", 2)
    for side in range(2):
        pieces[1, side] = exchanged(pieces[0, side], "expert", 1)
        pieces[3, side] = exchanged(pieces[2, side], "expert", 1)
    return pieces


def body(
    move,
    tokens,
    routes,
    combine_weight,
    w_in,
    w_out,
    grad_in,
    grad_out,
    first_in,
    second_in,
    first_out,
    second_out,
):
    device_count = lax.axis_size("expert")
    expert_count = device_count // GROUP
    token_count, route_count = routes.shape
    width = tokens.shape[1]
    half = width // 2
    capacity = GROUP * (
        (token_count * route_count * 4 + 3 * expert_count * GROUP - 1) // (3 * expert_count * GROUP)
    )
    dp_index = lax.axis_index("dp")
    my_group = lax.axis_index("expert") // GROUP

    flat_routes = routes.reshape(-1)
    ranks = slot_ranks(flat_routes, expert_count)
    relative = flat_routes ^ my_group
    targets = (relative * capacity + ranks).reshape(token_count, route_count)
    slot_ids = jnp.arange(expert_count * capacity, dtype=jnp.int32)
    selector = jnp.any(targets[None, :, :] == slot_ids[:, None, None], axis=2).astype(jnp.bfloat16)
    outgoing = jnp.dot(selector, tokens, preferred_element_type=jnp.float32).astype(jnp.bfloat16)
    outgoing = outgoing.reshape(expert_count, capacity, width)
    arrived = [outgoing[0]] + [
        exchanged(outgoing[mask], "expert", mask * GROUP) for mask in range(1, expert_count)
    ]

    weights = (w_in[0], w_in[1], w_out)
    gradients = (grad_in[0, 0], grad_in[0, 1], grad_out[0])
    firsts = (first_in[0], first_in[1], first_out)
    seconds = (second_in[0], second_in[1], second_out)
    sums = [summed_half(gradient, dp_index) for gradient in gradients]
    stepped = [adam_update(*arrays) for arrays in zip(weights, sums, firsts, seconds)]
    gate_pieces, up_pieces, out_pieces = [gathered(step[0]) for step in stepped]
    moved_first = [move(step[1]) for step in stepped]
    moved_second = [move(step[2]) for step in stepped]

    rows = jnp.concatenate(arrived, 0)
    sides = [
        lax.dynamic_slice_in_dim(rows, dp_index * half, half, 1),
        lax.dynamic_slice_in_dim(rows, (1 - dp_index) * half, half, 1),
    ]
    totals = [jnp.zeros((rows.shape[0], half), jnp.float32) for _ in range(2)]
    for quarter in (0, 1, 2, 3):
        gate = times_rows(sides[0], gate_pieces[quarter, 0]) + times_rows(
            sides[1], gate_pieces[quarter, 1]
        )
        upward = times_rows(sides[0], up_pieces[quarter, 0]) + times_rows(
            sides[1], up_pieces[quarter, 1]
        )
        hidden = (jax.nn.silu(gate) * upward).astype(jnp.bfloat16)
        for side in range(2):
            part = jnp.dot(
                hidden, out_pieces[quarter, side], preferred_element_type=jnp.float32
            ).astype(jnp.bfloat16)
            totals[side] = totals[side] + part.astype(jnp.float32)
    near, far = [total.astype(jnp.bfloat16) for total in totals]
    results = jnp.where(
        dp_index == 0, jnp.concatenate([near, far], 1), jnp.concatenate([far, near], 1)
    ).reshape(expert_count, capacity, width)
    returned = [results[0]] + [
        exchanged(results[mask], "expert", mask * GROUP) for mask in range(1, expert_count)
    ]
    by_slot = jnp.concatenate(returned, 0)
    weight_table = jnp.sum(
        jnp.where(targets[:, :, None] == slot_ids[None, None, :], combine_weight[:, :, None], 0.0),
        axis=1,
    )
    weight_high = weight_table.astype(jnp.bfloat16)
    weight_low = (weight_table - weight_high.astype(jnp.float32)).astype(jnp.bfloat16)
    combined = (
        jnp.dot(weight_high, by_slot, preferred_element_type=jnp.float32)
        + jnp.dot(weight_low, by_slot, preferred_element_type=jnp.float32)
    ).astype(jnp.bfloat16)
    return (
        combined,
        jnp.stack(moved_first[:2]),
        jnp.stack(moved_second[:2]),
        moved_first[2],
        moved_second[2],
    )


def local(tokens, routes, combine_weight, owner_plan, *state):
    device_count = lax.axis_size("expert")
    expert_count = device_count // GROUP
    operands = (tokens, routes, combine_weight) + state
    if expert_count == PLANES and lax.axis_size("dp") == 2:
        branches = [functools.partial(layer_call, mask) for mask in range(1, expert_count)]
        return store_call(lax.switch(owner_plan[0] - 1, branches, *operands))
    device_ids = jnp.arange(device_count, dtype=jnp.int32)
    source_rows = jnp.take(owner_plan, device_ids // GROUP) * GROUP + device_ids % GROUP
    return body(lambda moment: migrate_any(moment, source_rows, device_count), *operands)


def solution(mesh):
    in_specs = (
        P(("expert", "dp"), None),
        P(("expert", "dp"), None),
        P(("expert", "dp"), None),
        P(),
        P(None, "expert", "dp"),
        P("expert", "dp"),
        P("dp", None, "expert", None),
        P("dp", "expert", None),
        P(None, "expert", "dp"),
        P(None, "expert", "dp"),
        P("expert", "dp"),
        P("expert", "dp"),
    )
    out_specs = (
        P(("expert", "dp"), None),
        P(None, "expert", "dp"),
        P(None, "expert", "dp"),
        P("expert", "dp"),
        P("expert", "dp"),
    )
    return jax.shard_map(local, mesh=mesh, in_specs=in_specs, out_specs=out_specs, check_vma=False)
```
